32 devices in a mesh: dp: 16 (over z, x, core), tensor: 2 (over y).
Axes of the slice: x: 2, y: 2, z: 4, core: 2. Of those that a mesh axis runs over, the one named last changes fastest.
Arguments:
- hidden_in: bfloat16 [4096, 2048], P('dp'), may hold values from -6 to 6
- segments: int32 [16, 256], P('dp'), may hold values from 0 to 3, never falling along the last dimension, each value on 1 to 128 neighbouring positions
- expert_ids: int32 [4096, 6], P('dp'), may hold values from 0 to 15, all different within a row; in each aligned block of 256 rows (0 to 255, 256 to 511, ...) at most 144 rows name the same one
- grad_out: bfloat16 [4096, 2048], P('dp'), may hold values from -6 to 6
- attn_gain: bfloat16 [2048], P('dp'), may hold values from 0.5 to 1.5
- query_proj: bfloat16 [2048, 3072], P('dp', 'tensor'), may hold values from -0.125 to 0.125
- latent_down: bfloat16 [2048, 576], P('dp'), may hold values from -0.125 to 0.125
- latent_gain: bfloat16 [512], P('dp'), may hold values from 0.5 to 1.5
- latent_up: bfloat16 [512, 4096], P('dp', 'tensor'), may hold values from -0.25 to 0.25
- output_proj: bfloat16 [2048, 2048], P('tensor', 'dp'), may hold values from -0.375 to 0.375
- ffn_gain: bfloat16 [2048], P('dp'), may hold values from 0.5 to 1.5
- router_weight: bfloat16 [2048, 16], P('dp'), may hold values from -0.125 to 0.125
- shared_gate: bfloat16 [2048, 2816], P('dp', 'tensor'), may hold values from -0.125 to 0.125
- shared_up: bfloat16 [2048, 2816], P('dp', 'tensor'), may hold values from -0.125 to 0.125
- shared_down: bfloat16 [2816, 2048], P('tensor', 'dp'), may hold values from -0.109375 to 0.109375
- routed_gate_weight: bfloat16 [16, 2048, 1408], P('dp', None, 'tensor'), may hold values from -0.125 to 0.125
- routed_up_weight: bfloat16 [16, 2048, 1408], P('dp', None, 'tensor'), may hold values from -0.125 to 0.125
- routed_down_weight: bfloat16 [16, 1408, 2048], P('dp', 'tensor'), may hold values from -1 to 1
Outputs:
- output: bfloat16 [4096, 2048], P('dp')
- hidden_input_gradient: float32 [4096, 2048], P('dp')
- attention_gain_gradient: float32 [2048], P('dp')
- query_projection_gradient: float32 [2048, 3072], P('dp', 'tensor')
- latent_down_gradient: float32 [2048, 576], P('dp')
- grad_latent_gain: float32 [512], P('dp')
- grad_latent_up: float32 [512, 4096], P('dp', 'tensor')
- output_projection_gradient: float32 [2048, 2048], P('tensor', 'dp')
- feedforward_gain_gradient: float32 [2048], P('dp')
- router_weight_gradient: float32 [2048, 16], P('dp')
- grad_shared_gate: float32 [2048, 2816], P('dp', 'tensor')
- grad_shared_up: float32 [2048, 2816], P('dp', 'tensor')
- grad_shared_down: float32 [2816, 2048], P('tensor', 'dp')
- grad_expert_gate: float32 [16, 2048, 1408], P('dp', None, 'tensor')
- grad_expert_up: float32 [16, 2048, 1408], P('dp', None, 'tensor')
- grad_expert_down: float32 [16, 1408, 2048], P('dp', 'tensor')
The draws below stay inside these ranges and needn't reach their ends.
Inputs may be any that keep to these rules, and one draw needn't show every extreme that they name: `expert_ids`: each row names 6 different experts. Within the rows of one device (aligned blocks of 256 rows) no expert is named by more than 144 rows, a bound that some block reaches. `segments`: segment numbers never fall along a sequence; a segment has 1 to 128 positions.
All inputs are finite; a program needn't handle non-finite values.
Results may differ from the reference program's by a relative error of at most 0.02.
Values may be sent and summed in bfloat16 or wider, within the bound.
A program may use at most 320 MiB of HBM per device.

```python
import math
from functools import partial
import jax
import jax.numpy as jnp
import numpy as np
from jax import lax

D = 2048
H = 16
NOPE = 128
ROPE = 64
DV = 128
LAT = 512
FF_E = 1408
FF_S = 2816
TOPK = 6
LEN = 256
DOCS = 4
SEQ_DEV = 1
EXPERTS = 16
TOK_DEV = 256
SEQS = 16
TOKENS = 4096
CAP = 144
N_DP = 16
N_TENSOR = 2


def levels(key, extent, shards, least, largest):
    level, own = 1.0, jax.random.fold_in(key, 6)
    for position, blocks in shards:
        heights = jnp.exp(jax.random.uniform(jax.random.fold_in(own, position), (blocks,), jnp.float32, least / len(shards), largest / len(shards)))
        level = level * jnp.repeat(heights, extent[position] // blocks).reshape([-1 if axis == position else 1 for axis in range(len(extent))])
    return level


def length_profile(number_of, total, bound, lean):
    loads = [(1 << 20) // math.isqrt(standing ** lean) + 1 for standing in range(2, number_of + 1)]
    surplus, given = total - bound - (number_of - 1), [1] * (number_of - 1)
    while surplus > 0:
        free = [i for i in range(number_of - 1) if given[i] < bound]
        pool, left = sum([loads[i] for i in free]), surplus
        for i in free:
            extra = min(bound - given[i], max(1, left * loads[i] // pool), surplus)
            given[i] = given[i] + extra
            surplus = surplus - extra
    return np.array([bound] + given)


def uneven_parts(stream_key, amount, total, limit, skew):
    if amount == 2:
        one = jax.random.randint(stream_key, (), max(1, total - limit), min(limit, total - 1) + 1)
        return jnp.stack([one, total - one])
    sizes = jnp.asarray(length_profile(amount, total, limit, skew), jnp.int32)
    twos = (amount - 1) // 2
    giver, sink = sizes[1:1 + 2 * twos:2], sizes[2:2 + 2 * twos:2]
    slack = jnp.minimum(giver - 1, limit - sink)
    passed = jax.random.randint(jax.random.fold_in(stream_key, 1), (twos,), 0, 1 << 20) % (slack + 1)
    sizes = sizes.at[1:1 + 2 * twos:2].set(giver - passed).at[2:2 + 2 * twos:2].set(sink + passed)
    return sizes[jax.random.permutation(jax.random.fold_in(stream_key, 2), amount)]


def assign_block(stream_key, own, number, rows, amount, top, most, lean):
    ranking = jax.random.permutation(stream_key, amount)
    crowded, usual = portions_of(amount, rows * top, most, lean, True), portions_of(amount, rows * top, most, lean, False)
    places = jnp.arange(amount)

    def named(lengths, rotation):
        used = int((lengths > 0).sum())
        fixed = max(1, used // 4)
        passed = fixed + (places - fixed + rotation * (used - fixed)) % max(1, amount - fixed)
        return jnp.zeros((amount,), jnp.int32).at[ranking[jnp.where(places < fixed, places, passed)]].set(jnp.asarray(lengths, jnp.int32))

    lengths = jnp.where(number % 4 == 0, named(crowded, number // 4), named(usual, number - number // 4 - 1))
    mixed = jax.random.permutation(jax.random.fold_in(own, 3), amount)
    source_of, receiver = mixed[0:amount // 2 * 2:2], mixed[1:amount // 2 * 2:2]
    margin = jnp.minimum(lengths[source_of] - 1, most - lengths[receiver]) // 2
    margin = jnp.where((source_of == ranking[0]) | (receiver == ranking[0]) | (lengths[receiver] == 0), 0, jnp.maximum(margin, 0))
    passed = jax.random.randint(jax.random.fold_in(own, 4), (amount // 2,), 0, 1 << 20) % (margin + 1)
    lengths = lengths.at[source_of].add(-passed).at[receiver].add(passed)
    items = jnp.searchsorted(jnp.cumsum(lengths), jnp.arange(rows * top), side="right").astype(jnp.int32)
    table = items.reshape(top, rows).T
    table = table[jax.random.permutation(jax.random.fold_in(own, 1), rows)]
    rotation = jax.random.randint(jax.random.fold_in(own, 2), (rows, 1), 0, top)
    return jnp.take_along_axis(table, (jnp.arange(top)[None, :] + rotation) % top, axis=1)


def portions_of(amount, total, most, skew, full):
    loads = [(1 << 20) // math.isqrt(standing ** skew) + 1 for standing in range(1, amount + 1)]
    largest = most if full else min(most, max(-(-total // amount), total * loads[0] // sum(loads)))
    least = 1 if total - largest >= amount - 1 else 0
    counts, surplus = [largest] + [least] * (amount - 1), total - largest - least * (amount - 1)
    while surplus > 0:
        candidates = [i for i in range(1, amount) if counts[i] < largest] or [i for i in range(1, amount) if counts[i] < most]
        mass, left = sum([loads[i] for i in candidates]), surplus
        for i in candidates:
            addition = min(most - counts[i], max(1, left * loads[i] // mass), surplus)
            counts[i] = counts[i] + addition
            surplus = surplus - addition
    return np.array(counts)


def gaussian(stream_key, extent, spread, limit, pieces=(), held_as=jnp.bfloat16):
    level = levels(stream_key, extent, pieces, -0.22, 0.18) if pieces else 1.0
    drawn = jax.random.normal(stream_key, extent, jnp.float32) * spread * level
    return jnp.minimum(jnp.maximum(drawn, -limit), limit).astype(held_as)


def setup_inputs(seed: int = 0) -> dict:
    keys = jax.random.split(jax.random.key(seed), 19)
    hidden_in = gaussian(keys[0], (TOKENS, D), 1.0, 6.0, ((0, 16),))
    segments = jax.vmap(lambda own: jnp.searchsorted(jnp.cumsum(uneven_parts(own, DOCS, LEN, LEN // 2, 0)), jnp.arange(LEN), side="right"))(jax.random.split(keys[1], SEQS)).reshape((SEQS, LEN)).astype(jnp.int32)
    expert_ids_keys = jax.random.split(jax.random.fold_in(keys[2], 1), TOKENS // TOK_DEV)
    expert_ids_turns = jax.random.permutation(jax.random.fold_in(keys[2], 3), TOKENS // TOK_DEV)
    expert_ids = jax.vmap(lambda own, number: assign_block(jax.random.fold_in(keys[2], 2), own, number, TOK_DEV, EXPERTS, TOPK, CAP, 2))(expert_ids_keys, expert_ids_turns).reshape((TOKENS, TOPK))
    grad_out = gaussian(keys[3], (TOKENS, D), 1.0, 6.0, ((0, 16),))
    attn_gain = jnp.clip(1.0 + 0.1 * jax.random.normal(keys[4], (D,), jnp.float32), 0.5, 1.5).astype(jnp.bfloat16)
    query_proj = gaussian(keys[5], (D, H * (NOPE + ROPE)), D ** -0.5, 0.125, ((0, 16), (1, 2)))
    latent_down = gaussian(keys[6], (D, LAT + ROPE), D ** -0.5, 0.125, ((0, 16),))
    latent_gain = jnp.clip(1.0 + 0.1 * jax.random.normal(keys[7], (LAT,), jnp.float32), 0.5, 1.5).astype(jnp.bfloat16)
    latent_up = gaussian(keys[8], (LAT, H * (NOPE + DV)), LAT ** -0.5, 0.25, ((0, 16), (1, 2)))
    output_proj = gaussian(keys[9], (H * DV, D), (H * DV // 8) ** -0.5, 0.375, ((0, 2), (1, 16)))
    ffn_gain = jnp.clip(1.0 + 0.1 * jax.random.normal(keys[10], (D,), jnp.float32), 0.5, 1.5).astype(jnp.bfloat16)
    router_weight = gaussian(keys[11], (D, EXPERTS), D ** -0.5, 0.125, ((0, 16),))
    shared_gate = gaussian(keys[12], (D, FF_S), D ** -0.5, 0.125, ((0, 16), (1, 2)))
    shared_up = gaussian(keys[13], (D, FF_S), D ** -0.5, 0.125, ((0, 16), (1, 2)))
    shared_down = gaussian(keys[14], (FF_S, D), FF_S ** -0.5, 0.109375, ((0, 2), (1, 16)))
    routed_gate_weight = gaussian(keys[15], (EXPERTS, D, FF_E), D ** -0.5, 0.125, ((0, 16), (2, 2)))
    routed_up_weight = gaussian(keys[16], (EXPERTS, D, FF_E), D ** -0.5, 0.125, ((0, 16), (2, 2)))
    routed_down_weight = gaussian(keys[17], (EXPERTS, FF_E, D), (FF_E // 36) ** -0.5, 1.0, ((0, 16), (1, 2)))
    return dict(hidden_in=hidden_in, segments=segments, expert_ids=expert_ids, grad_out=grad_out, attn_gain=attn_gain, query_proj=query_proj, latent_down=latent_down, latent_gain=latent_gain, latent_up=latent_up, output_proj=output_proj, ffn_gain=ffn_gain, router_weight=router_weight, shared_gate=shared_gate, shared_up=shared_up, shared_down=shared_down, routed_gate_weight=routed_gate_weight, routed_up_weight=routed_up_weight, routed_down_weight=routed_down_weight)


EPS = 1e-06
ROPE_BASE = 10000.0
NEG_FILL = -1e+30

def rope_tables(length, width):
    half_width = width // 2
    frequency = ROPE_BASE ** (-(jnp.arange(half_width, dtype=jnp.float32) * (2.0 / width)))
    angles = jnp.arange(length, dtype=jnp.float32)[:, None] * frequency[None, :]
    angles = jnp.concatenate([angles, angles], axis=1)
    return (jnp.cos(angles), jnp.sin(angles))

def rotate(values, cos_table, sin_table):
    half_width = values.shape[-1] // 2
    turned = jnp.concatenate([-values[..., half_width:], values[..., :half_width]], axis=-1)
    return values * cos_table + turned * sin_table

def rms_recip(values):
    return lax.rsqrt(lax.optimization_barrier(jnp.mean(values * values, axis=-1, keepdims=True)) + EPS)

def rms_back(grad_normed, values, recip, gain):
    hat_values = values * recip
    scaled = grad_normed * gain
    grad_in = recip * (scaled - hat_values * lax.optimization_barrier(jnp.mean(scaled * hat_values, axis=-1, keepdims=True)))
    grad_gain = lax.optimization_barrier(jnp.sum(grad_normed * hat_values, axis=0))
    return (grad_in, grad_gain)

def silu_parts(pre_act):
    sigmoid_val = jax.nn.sigmoid(pre_act)
    return (pre_act * sigmoid_val, sigmoid_val * (1.0 + pre_act * (1.0 - sigmoid_val)))

def slot_positions(chosen, experts):
    matches = (chosen[:, :, None] == jnp.arange(experts, dtype=jnp.int32)).astype(jnp.int32).reshape(-1, experts)
    earlier = jnp.cumsum(matches, axis=0) - matches
    return lax.optimization_barrier(jnp.sum(earlier * matches, axis=1)).reshape(chosen.shape)

def mask_table(segments):
    places = jnp.arange(segments.shape[1], dtype=jnp.int32)
    same_doc = segments[:, :, None] == segments[:, None, :]
    return same_doc & (places[None, None, :] <= places[None, :, None])

def attend_scores(query_all, key_nope, key_rope, allowed):
    nope_width = key_nope.shape[-1]
    scale = query_all.shape[-1] ** (-0.5)
    query_all = query_all.astype(jnp.float32)
    scores = jnp.einsum('sqhd,skhd->shqk', query_all[..., :nope_width], key_nope.astype(jnp.float32))
    scores = scores + jnp.einsum('sqhd,skd->shqk', query_all[..., nope_width:], key_rope.astype(jnp.float32))
    return jnp.where(allowed[:, None], scores * scale, NEG_FILL)

def attend_forward(bundle):
    query_all, key_nope, key_rope, values, segs = bundle
    allowed = mask_table(segs)
    scores = attend_scores(query_all, key_nope, key_rope, allowed)
    highest = lax.optimization_barrier(jnp.max(scores, axis=-1, keepdims=True))
    log_total = highest + jnp.log(lax.optimization_barrier(jnp.sum(jnp.exp(scores - highest), axis=-1, keepdims=True)))
    attn_probs = jnp.exp(scores - log_total).astype(jnp.bfloat16)
    heads_out = jnp.einsum('shqk,skhd->sqhd', attn_probs.astype(jnp.float32), values.astype(jnp.float32)).astype(jnp.bfloat16)
    return (heads_out, log_total)

def attend_backward(bundle):
    query_all, key_nope, key_rope, values, segs, heads_out, log_total, heads_grad = bundle
    nope_width = key_nope.shape[-1]
    scale = query_all.shape[-1] ** (-0.5)
    allowed = mask_table(segs)
    scores = attend_scores(query_all, key_nope, key_rope, allowed)
    attn_probs = jnp.exp(scores - log_total)
    probs_low = attn_probs.astype(jnp.bfloat16).astype(jnp.float32)
    grad_float = heads_grad.astype(jnp.float32)
    values_grad = jnp.einsum('shqk,sqhd->skhd', probs_low, grad_float)
    probs_grad = jnp.einsum('sqhd,skhd->shqk', grad_float, values.astype(jnp.float32))
    delta = lax.optimization_barrier(jnp.sum(grad_float * heads_out.astype(jnp.float32), axis=-1))
    delta = jnp.transpose(delta, (0, 2, 1))[..., None]
    score_grad = (attn_probs * (probs_grad - delta) * scale).astype(jnp.bfloat16).astype(jnp.float32)
    query_float = query_all.astype(jnp.float32)
    nope_grad_q = jnp.einsum('shqk,skhd->sqhd', score_grad, key_nope.astype(jnp.float32))
    rope_grad_q = jnp.einsum('shqk,skd->sqhd', score_grad, key_rope.astype(jnp.float32))
    key_nope_grad = jnp.einsum('shqk,sqhd->skhd', score_grad, query_float[..., :nope_width])
    key_rope_grad = jnp.einsum('shqk,sqhd->skd', score_grad, query_float[..., nope_width:])
    return (jnp.concatenate([nope_grad_q, rope_grad_q], axis=-1), key_nope_grad, values_grad, key_rope_grad)

def reference(hidden_in, segments, expert_ids, grad_out, attn_gain, query_proj, latent_down, latent_gain, latent_up, output_proj, ffn_gain, router_weight, shared_gate, shared_up, shared_down, routed_gate_weight, routed_up_weight, routed_down_weight):
    float_type = jnp.float32
    low_type = jnp.bfloat16
    head_dim = NOPE + ROPE

    def by_group(array):
        return array.reshape((N_DP, SEQ_DEV, LEN) + array.shape[1:])

    def from_group(array):
        return array.reshape((TOKENS,) + array.shape[3:])
    residual_in = hidden_in.astype(float_type)
    recip_one = rms_recip(residual_in)
    normed_one = (residual_in * recip_one * attn_gain.astype(float_type)).astype(low_type)
    cos_table, sin_table = rope_tables(LEN, ROPE)
    cos_tok = jnp.tile(cos_table, (SEQS, 1))
    sin_tok = jnp.tile(sin_table, (SEQS, 1))
    query_raw = jnp.dot(normed_one, query_proj, preferred_element_type=float_type).reshape(TOKENS, H, head_dim)
    queries = jnp.concatenate([query_raw[..., :NOPE], rotate(query_raw[..., NOPE:], cos_tok[:, None], sin_tok[:, None])], axis=-1).astype(low_type)
    down_raw = jnp.dot(normed_one, latent_down, preferred_element_type=float_type)
    latent = down_raw[:, :LAT]
    recip_latent = rms_recip(latent)
    latent_normed = (latent * recip_latent * latent_gain.astype(float_type)).astype(low_type)
    key_rope = rotate(down_raw[:, LAT:], cos_tok, sin_tok).astype(low_type)
    keys_values = jnp.dot(latent_normed, latent_up, preferred_element_type=float_type).astype(low_type).reshape(TOKENS, H, NOPE + DV)
    key_nope = keys_values[..., :NOPE]
    values = keys_values[..., NOPE:]
    seg_groups = segments.reshape(N_DP, SEQ_DEV, LEN)
    heads_out, log_total = lax.map(attend_forward, (by_group(queries), by_group(key_nope), by_group(key_rope), by_group(values), seg_groups))
    attn_flat = from_group(heads_out).reshape(TOKENS, H * DV)
    mid = residual_in + jnp.dot(attn_flat, output_proj, preferred_element_type=float_type)
    recip_two = rms_recip(mid)
    normed_two = (mid * recip_two * ffn_gain.astype(float_type)).astype(low_type)
    logits = jnp.dot(normed_two, router_weight, preferred_element_type=float_type)
    router_probs = jax.nn.softmax(logits, axis=-1)
    selector = (expert_ids[:, :, None] == jnp.arange(EXPERTS, dtype=jnp.int32)).astype(float_type)
    gate_weight = lax.optimization_barrier(jnp.sum(selector * router_probs[:, None, :], axis=-1))
    shared_pre_gate = jnp.dot(normed_two, shared_gate, preferred_element_type=float_type)
    shared_pre_up = jnp.dot(normed_two, shared_up, preferred_element_type=float_type)
    shared_act, shared_slope = silu_parts(shared_pre_gate)
    shared_hidden = (shared_act * shared_pre_up).astype(low_type)
    shared_out = jnp.dot(shared_hidden, shared_down, preferred_element_type=float_type)
    grad_float = grad_out.astype(float_type)
    slots = jax.vmap(partial(slot_positions, experts=EXPERTS))(expert_ids.reshape(N_DP, TOK_DEV, TOPK)).reshape(TOKENS, TOPK)
    source = (jnp.arange(TOKENS, dtype=jnp.int32) // TOK_DEV)[:, None]
    columns = source * CAP + slots
    choice_count = TOKENS * TOPK
    choice_ids = jnp.arange(choice_count, dtype=jnp.int32).reshape(TOKENS, TOPK)
    lookup_grid = jnp.full((EXPERTS, N_DP * CAP), choice_count, jnp.int32).at[expert_ids, columns].set(choice_ids)
    gate_flat = gate_weight.reshape(-1)

    def routed_expert_sweep(carry, slab):
        mixture_total, mixture_gradient, weight_grad = carry
        row_ids, gate_w, up_w, down_w = slab
        is_live = row_ids < choice_count
        safe_ids = jnp.minimum(row_ids, choice_count - 1)
        token_of = safe_ids // TOPK
        target = jnp.where(is_live, token_of, TOKENS)
        token_rows = jnp.where(is_live[:, None], normed_two[token_of], jnp.zeros((), low_type))
        pre_gate = jnp.dot(token_rows, gate_w, preferred_element_type=float_type)
        pre_up = jnp.dot(token_rows, up_w, preferred_element_type=float_type)
        act_value, slope = silu_parts(pre_gate)
        hidden = (act_value * pre_up).astype(low_type)
        part_width = hidden.shape[1] // N_TENSOR
        combined = jnp.zeros((hidden.shape[0], down_w.shape[1]), float_type)
        for group in range(N_TENSOR):
            lower = group * part_width
            upper = lower + part_width
            piece = jnp.dot(hidden[:, lower:upper], down_w[lower:upper], preferred_element_type=float_type).astype(low_type)
            combined = combined + lax.optimization_barrier(piece).astype(float_type)
        gate_of = jnp.where(is_live, gate_flat[safe_ids], 0.0)
        mixture_total = mixture_total.at[target].add(gate_of[:, None] * combined, mode='drop')
        grad_rows = grad_float[token_of]
        weight_grad = weight_grad.at[jnp.where(is_live, safe_ids, choice_count)].add(lax.optimization_barrier(jnp.sum(grad_rows * combined, axis=1)), mode='drop')
        slot_grad = (gate_of[:, None] * grad_rows).astype(low_type)
        hidden_grad = jnp.dot(slot_grad, down_w.T, preferred_element_type=float_type)
        pre_gate_grad = (hidden_grad * pre_up * slope).astype(low_type)
        pre_up_grad = (hidden_grad * act_value).astype(low_type)
        grad_down_w = jnp.dot(hidden.T, slot_grad, preferred_element_type=float_type)
        grad_gate_w = jnp.dot(token_rows.T, pre_gate_grad, preferred_element_type=float_type)
        grad_up_w = jnp.dot(token_rows.T, pre_up_grad, preferred_element_type=float_type)
        row_grad = jnp.zeros((hidden.shape[0], down_w.shape[1]), float_type)
        for group in range(N_TENSOR):
            lower = group * part_width
            upper = lower + part_width
            piece = jnp.dot(pre_gate_grad[:, lower:upper], gate_w[:, lower:upper].T, preferred_element_type=float_type)
            piece = piece + jnp.dot(pre_up_grad[:, lower:upper], up_w[:, lower:upper].T, preferred_element_type=float_type)
            row_grad = row_grad + lax.optimization_barrier(piece.astype(low_type)).astype(float_type)
        mixture_gradient = mixture_gradient.at[target].add(row_grad, mode='drop')
        return ((mixture_total, mixture_gradient, weight_grad), (grad_gate_w, grad_up_w, grad_down_w))
    initial_loop_state = (jnp.zeros((TOKENS, D), float_type), jnp.zeros((TOKENS, D), float_type), jnp.zeros((choice_count,), float_type))
    (mixture_total, mixture_gradient, flattened_weight), (routed_gate_gradient, routed_up_gradient, routed_down_gradient) = lax.scan(routed_expert_sweep, initial_loop_state, (lookup_grid, routed_gate_weight, routed_up_weight, routed_down_weight))
    output = (mid + shared_out + mixture_total).astype(low_type)
    shared_act_grad = jnp.dot(grad_out, shared_down.T, preferred_element_type=float_type)
    shared_gate_grad = (shared_act_grad * shared_pre_up * shared_slope).astype(low_type)
    shared_up_grad = (shared_act_grad * shared_act).astype(low_type)
    shared_down_gradient = jnp.dot(shared_hidden.T, grad_out, preferred_element_type=float_type)
    shared_gate_gradient = jnp.dot(normed_two.T, shared_gate_grad, preferred_element_type=float_type)
    shared_up_gradient = jnp.dot(normed_two.T, shared_up_grad, preferred_element_type=float_type)
    normed_two_grad = jnp.dot(shared_gate_grad, shared_gate.T, preferred_element_type=float_type)
    normed_two_grad = normed_two_grad + jnp.dot(shared_up_grad, shared_up.T, preferred_element_type=float_type)
    normed_two_grad = normed_two_grad + mixture_gradient
    weight_grad = flattened_weight.reshape(TOKENS, TOPK)
    prob_grad = lax.optimization_barrier(jnp.sum(selector * weight_grad[:, :, None], axis=1))
    logit_grad = (router_probs * (prob_grad - lax.optimization_barrier(jnp.sum(prob_grad * router_probs, axis=-1, keepdims=True)))).astype(low_type)
    router_weight_gradient = jnp.dot(normed_two.T, logit_grad, preferred_element_type=float_type)
    normed_two_grad = normed_two_grad + jnp.dot(logit_grad, router_weight.T, preferred_element_type=float_type)
    norm_two_back, feedforward_gain_gradient = rms_back(normed_two_grad, mid, recip_two, ffn_gain.astype(float_type))
    mid_grad = grad_float + norm_two_back
    mid_low = mid_grad.astype(low_type)
    output_projection_gradient = jnp.dot(attn_flat.T, mid_low, preferred_element_type=float_type)
    heads_grad = jnp.dot(mid_low, output_proj.T, preferred_element_type=float_type).astype(low_type).reshape(TOKENS, H, DV)
    query_grad, key_nope_grad, values_grad, key_rope_grad = lax.map(attend_backward, (by_group(queries), by_group(key_nope), by_group(key_rope), by_group(values), seg_groups, heads_out, log_total, by_group(heads_grad)))
    query_grad = from_group(query_grad)
    query_raw_grad = jnp.concatenate([query_grad[..., :NOPE], rotate(query_grad[..., NOPE:], cos_tok[:, None], -sin_tok[:, None])], axis=-1).astype(low_type).reshape(TOKENS, H * head_dim)
    query_projection_gradient = jnp.dot(normed_one.T, query_raw_grad, preferred_element_type=float_type)
    kv_grad = jnp.concatenate([from_group(key_nope_grad), from_group(values_grad)], axis=-1).astype(low_type).reshape(TOKENS, H * (NOPE + DV))
    latent_up_gradient = jnp.dot(latent_normed.T, kv_grad, preferred_element_type=float_type)
    latent_normed_grad = jnp.dot(kv_grad, latent_up.T, preferred_element_type=float_type)
    latent_grad, latent_gain_gradient = rms_back(latent_normed_grad, latent, recip_latent, latent_gain.astype(float_type))
    rope_pre_grad = rotate(from_group(key_rope_grad), cos_tok, -sin_tok)
    down_grad = jnp.concatenate([latent_grad, rope_pre_grad], axis=-1).astype(low_type)
    latent_down_gradient = jnp.dot(normed_one.T, down_grad, preferred_element_type=float_type)
    normed_one_grad = jnp.dot(query_raw_grad, query_proj.T, preferred_element_type=float_type)
    normed_one_grad = normed_one_grad + jnp.dot(down_grad, latent_down.T, preferred_element_type=float_type)
    norm_one_back, attention_gain_gradient = rms_back(normed_one_grad, residual_in, recip_one, attn_gain.astype(float_type))
    hidden_input_gradient = mid_grad + norm_one_back
    return (output, hidden_input_gradient, attention_gain_gradient, query_projection_gradient, latent_down_gradient, latent_gain_gradient, latent_up_gradient, output_projection_gradient, feedforward_gain_gradient, router_weight_gradient, shared_gate_gradient, shared_up_gradient, shared_down_gradient, routed_gate_gradient, routed_up_gradient, routed_down_gradient)
```

```python
import jax
import jax.numpy as jnp
from jax import lax
from jax.sharding import PartitionSpec as P

NOPE = 128
ROPE = 64
DV = 128
LAT = 512


EPS = 1e-06
ROPE_BASE = 10000.0
NEG_FILL = -1e30


def rope_tables(length, width):
    half_width = width // 2
    frequency = ROPE_BASE ** (-(jnp.arange(half_width, dtype=jnp.float32) * (2.0 / width)))
    angles = jnp.arange(length, dtype=jnp.float32)[:, None] * frequency[None, :]
    angles = jnp.concatenate([angles, angles], axis=1)
    return (jnp.cos(angles), jnp.sin(angles))


def rotate(values, cos_table, sin_table):
    half_width = values.shape[-1] // 2
    turned = jnp.concatenate([-values[..., half_width:], values[..., :half_width]], axis=-1)
    return values * cos_table + turned * sin_table


def rms_recip(values):
    return lax.rsqrt(jnp.mean(values * values, axis=-1, keepdims=True) + EPS)


def rms_back(grad_normed, values, recip, gain):
    hat_values = values * recip
    scaled = grad_normed * gain
    grad_in = recip * (scaled - hat_values * jnp.mean(scaled * hat_values, axis=-1, keepdims=True))
    grad_gain = jnp.sum(grad_normed * hat_values, axis=0)
    return (grad_in, grad_gain)


def silu_parts(pre_act):
    sigmoid_val = jax.nn.sigmoid(pre_act)
    return (pre_act * sigmoid_val, sigmoid_val * (1.0 + pre_act * (1.0 - sigmoid_val)))


def mask_table(segments):
    places = jnp.arange(segments.shape[1], dtype=jnp.int32)
    same_doc = segments[:, :, None] == segments[:, None, :]
    return same_doc & (places[None, None, :] <= places[None, :, None])


def attend_scores(query_all, key_nope, key_rope, allowed):
    nope_width = key_nope.shape[-1]
    scale = query_all.shape[-1] ** (-0.5)
    scores = jnp.einsum(
        "sqhd,skhd->shqk", query_all[..., :nope_width], key_nope, preferred_element_type=jnp.float32
    )
    scores = scores + jnp.einsum(
        "sqhd,skd->shqk", query_all[..., nope_width:], key_rope, preferred_element_type=jnp.float32
    )
    return jnp.where(allowed[:, None], scores * scale, NEG_FILL)


def slot_positions(chosen, experts):
    matches = (
        (chosen[:, :, None] == jnp.arange(experts, dtype=jnp.int32))
        .astype(jnp.int32)
        .reshape(-1, experts)
    )
    earlier = jnp.cumsum(matches, axis=0) - matches
    return jnp.sum(earlier * matches, axis=1).reshape(chosen.shape)


def to_expert(arrived, sources, local_count):
    capacity = arrived.shape[1]
    feature_width = arrived.shape[2]
    grouped = arrived.reshape(sources, local_count, capacity, feature_width)
    return jnp.transpose(grouped, (1, 0, 2, 3)).reshape(
        local_count, sources * capacity, feature_width
    )


def from_expert(expert_rows, sources):
    local_count = expert_rows.shape[0]
    capacity = expert_rows.shape[1] // sources
    feature_width = expert_rows.shape[2]
    grouped = expert_rows.reshape(local_count, sources, capacity, feature_width)
    return jnp.transpose(grouped, (1, 0, 2, 3)).reshape(
        sources * local_count, capacity, feature_width
    )


def local_exchanged(
    hidden_in,
    segments,
    expert_ids,
    grad_out,
    attn_gain,
    query_proj,
    latent_down,
    latent_gain,
    latent_up,
    output_proj,
    ffn_gain,
    router_weight,
    shared_gate,
    shared_up,
    shared_down,
    routed_gate_weight,
    routed_up_weight,
    routed_down_weight,
):
    float_type = jnp.float32
    low_type = jnp.bfloat16
    tok_count = hidden_in.shape[0]
    seq_count = segments.shape[0]
    seq_len = segments.shape[1]
    top_count = expert_ids.shape[1]
    head_dim = NOPE + ROPE
    dp_count = lax.axis_size("dp")
    local_experts = routed_gate_weight.shape[0]
    dense_weights = (
        attn_gain,
        query_proj,
        latent_down,
        latent_gain,
        latent_up,
        output_proj,
        ffn_gain,
        router_weight,
        shared_gate,
        shared_up,
        shared_down,
    )
    gathered = (
        lax.all_gather(dense_weights[0], "dp", axis=0, tiled=True),
        lax.all_gather(dense_weights[1], "dp", axis=0, tiled=True),
        lax.all_gather(dense_weights[2], "dp", axis=0, tiled=True),
        lax.all_gather(dense_weights[3], "dp", axis=0, tiled=True),
        lax.all_gather(dense_weights[4], "dp", axis=0, tiled=True),
        lax.all_gather(dense_weights[5], "dp", axis=1, tiled=True),
        lax.all_gather(dense_weights[6], "dp", axis=0, tiled=True),
        lax.all_gather(dense_weights[7], "dp", axis=0, tiled=True),
        lax.all_gather(dense_weights[8], "dp", axis=0, tiled=True),
        lax.all_gather(dense_weights[9], "dp", axis=0, tiled=True),
        lax.all_gather(dense_weights[10], "dp", axis=1, tiled=True),
    )
    (
        full_attn_gain,
        full_query,
        full_down,
        full_lgain,
        full_up,
        full_output,
        full_ffn_gain,
        full_router,
        full_sgate,
        full_sup,
        full_sdown,
    ) = gathered
    num_experts = full_router.shape[1]
    capacity = 3 * tok_count * top_count // (2 * num_experts)
    head_count = full_query.shape[1] // head_dim

    def by_seq(array):
        return array.reshape((seq_count, seq_len) + array.shape[1:])

    residual_in = hidden_in.astype(float_type)
    recip_one = rms_recip(residual_in)
    normed_one = (residual_in * recip_one * full_attn_gain.astype(float_type)).astype(low_type)
    cos_table, sin_table = rope_tables(seq_len, ROPE)
    cos_tok = jnp.tile(cos_table, (seq_count, 1))
    sin_tok = jnp.tile(sin_table, (seq_count, 1))
    query_raw = jnp.dot(normed_one, full_query, preferred_element_type=float_type).reshape(
        tok_count, head_count, head_dim
    )
    queries = jnp.concatenate(
        [query_raw[..., :NOPE], rotate(query_raw[..., NOPE:], cos_tok[:, None], sin_tok[:, None])],
        axis=-1,
    ).astype(low_type)
    down_raw = jnp.dot(normed_one, full_down, preferred_element_type=float_type)
    latent = down_raw[:, :LAT]
    recip_latent = rms_recip(latent)
    latent_normed = (latent * recip_latent * full_lgain.astype(float_type)).astype(low_type)
    key_rope = rotate(down_raw[:, LAT:], cos_tok, sin_tok).astype(low_type)
    keys_values = (
        jnp.dot(latent_normed, full_up, preferred_element_type=float_type)
        .astype(low_type)
        .reshape(tok_count, head_count, NOPE + DV)
    )
    key_nope = by_seq(keys_values[..., :NOPE])
    values = by_seq(keys_values[..., NOPE:])
    query_seq = by_seq(queries)
    rope_seq = by_seq(key_rope)
    allowed = mask_table(segments)
    scores = attend_scores(query_seq, key_nope, rope_seq, allowed)
    highest = jnp.max(scores, axis=-1, keepdims=True)
    log_total = highest + jnp.log(jnp.sum(jnp.exp(scores - highest), axis=-1, keepdims=True))
    attn_probs = jnp.exp(scores - log_total).astype(low_type)
    heads_out = jnp.einsum(
        "shqk,skhd->sqhd", attn_probs, values, preferred_element_type=float_type
    ).astype(low_type)
    attn_flat = heads_out.reshape(tok_count, head_count * DV)
    attn_part = jnp.dot(attn_flat, full_output, preferred_element_type=float_type)
    attn_full = lax.psum(attn_part, "tensor")
    mid = residual_in + attn_full
    recip_two = rms_recip(mid)
    normed_two = (mid * recip_two * full_ffn_gain.astype(float_type)).astype(low_type)
    logits = jnp.dot(normed_two, full_router, preferred_element_type=float_type)
    router_probs = jax.nn.softmax(logits, axis=-1)
    selector = (expert_ids[:, :, None] == jnp.arange(num_experts, dtype=jnp.int32)).astype(
        float_type
    )
    gate_weight = jnp.sum(selector * router_probs[:, None, :], axis=-1)
    shared_pre_gate = jnp.dot(normed_two, full_sgate, preferred_element_type=float_type)
    shared_pre_up = jnp.dot(normed_two, full_sup, preferred_element_type=float_type)
    shared_act, shared_slope = silu_parts(shared_pre_gate)
    shared_hidden = (shared_act * shared_pre_up).astype(low_type)
    shared_part = jnp.dot(shared_hidden, full_sdown, preferred_element_type=float_type)
    slots = slot_positions(expert_ids, num_experts)
    place_grid = expert_ids * capacity + slots
    places = place_grid.reshape(-1)
    place_rows = jnp.arange(num_experts * capacity, dtype=jnp.int32)
    dispatch_table = jnp.sum(
        (place_grid[None, :, :] == place_rows[:, None, None]).astype(low_type), axis=-1
    )
    send_rows = (
        jnp.dot(dispatch_table, normed_two, preferred_element_type=float_type)
        .astype(low_type)
        .reshape(num_experts, capacity, -1)
    )
    arrived = lax.all_to_all(send_rows, "dp", split_axis=0, concat_axis=0, tiled=True)
    expert_rows = to_expert(arrived, dp_count, local_experts)
    pre_gate = jnp.einsum(
        "erd,edf->erf", expert_rows, routed_gate_weight, preferred_element_type=float_type
    )
    pre_up = jnp.einsum(
        "erd,edf->erf", expert_rows, routed_up_weight, preferred_element_type=float_type
    )
    expert_act, expert_slope = silu_parts(pre_gate)
    expert_hidden = (expert_act * pre_up).astype(low_type)
    expert_result = jnp.einsum(
        "erf,efd->erd", expert_hidden, routed_down_weight, preferred_element_type=float_type
    ).astype(low_type)
    returned = lax.all_to_all(
        from_expert(expert_result, dp_count), "dp", split_axis=0, concat_axis=0, tiled=True
    )
    picked = (
        returned.reshape(num_experts * capacity, -1)[places]
        .reshape(tok_count, top_count, -1)
        .astype(float_type)
    )
    moe_part = jnp.sum(gate_weight[:, :, None] * picked, axis=1)
    ffn_full = lax.psum((moe_part + shared_part).astype(jnp.bfloat16), "tensor").astype(jnp.float32)
    output = (mid + ffn_full).astype(low_type)
    back_weights = (
        lax.all_gather(dense_weights[0], "dp", axis=0, tiled=True),
        lax.all_gather(dense_weights[1], "dp", axis=0, tiled=True),
        lax.all_gather(dense_weights[2], "dp", axis=0, tiled=True),
        lax.all_gather(dense_weights[3], "dp", axis=0, tiled=True),
        lax.all_gather(dense_weights[4], "dp", axis=0, tiled=True),
        lax.all_gather(dense_weights[5], "dp", axis=1, tiled=True),
        lax.all_gather(dense_weights[6], "dp", axis=0, tiled=True),
        lax.all_gather(dense_weights[7], "dp", axis=0, tiled=True),
        lax.all_gather(dense_weights[8], "dp", axis=0, tiled=True),
        lax.all_gather(dense_weights[9], "dp", axis=0, tiled=True),
        lax.all_gather(dense_weights[10], "dp", axis=1, tiled=True),
    )
    (
        back_attn_gain,
        back_query,
        back_down,
        back_lgain,
        back_up,
        back_output,
        back_ffn_gain,
        back_router,
        back_sgate,
        back_sup,
        back_sdown,
    ) = back_weights
    grad_float = grad_out.astype(float_type)
    shared_act_grad = jnp.dot(grad_out, back_sdown.T, preferred_element_type=float_type)
    shared_gate_grad = (shared_act_grad * shared_pre_up * shared_slope).astype(low_type)
    shared_up_grad = (shared_act_grad * shared_act).astype(low_type)
    shared_down_gradient = jnp.dot(shared_hidden.T, grad_out, preferred_element_type=float_type)
    shared_gate_gradient = jnp.dot(
        normed_two.T, shared_gate_grad, preferred_element_type=float_type
    )
    shared_up_gradient = jnp.dot(normed_two.T, shared_up_grad, preferred_element_type=float_type)
    shared_in_grad = jnp.dot(shared_gate_grad, back_sgate.T, preferred_element_type=float_type)
    shared_in_grad = shared_in_grad + jnp.dot(
        shared_up_grad, back_sup.T, preferred_element_type=float_type
    )
    weight_grad_part = jnp.sum(grad_float[:, None, :] * picked, axis=-1)
    slot_grad = (
        (gate_weight[:, :, None] * grad_float[:, None, :])
        .astype(low_type)
        .reshape(tok_count * top_count, -1)
    )
    grad_send = (
        jnp.zeros((num_experts * capacity, slot_grad.shape[1]), low_type)
        .at[places]
        .set(slot_grad)
        .reshape(num_experts, capacity, -1)
    )
    grad_arrived = to_expert(
        lax.all_to_all(grad_send, "dp", split_axis=0, concat_axis=0, tiled=True),
        dp_count,
        local_experts,
    )
    hidden_grad = jnp.einsum(
        "erd,efd->erf", grad_arrived, routed_down_weight, preferred_element_type=float_type
    )
    pre_gate_grad = (hidden_grad * pre_up * expert_slope).astype(low_type)
    pre_up_grad = (hidden_grad * expert_act).astype(low_type)
    routed_down_gradient = jnp.einsum(
        "erf,erd->efd", expert_hidden, grad_arrived, preferred_element_type=float_type
    )
    routed_gate_gradient = jnp.einsum(
        "erd,erf->edf", expert_rows, pre_gate_grad, preferred_element_type=float_type
    )
    routed_up_gradient = jnp.einsum(
        "erd,erf->edf", expert_rows, pre_up_grad, preferred_element_type=float_type
    )
    row_grad = jnp.einsum(
        "erf,edf->erd", pre_gate_grad, routed_gate_weight, preferred_element_type=float_type
    )
    row_grad = (
        row_grad
        + jnp.einsum(
            "erf,edf->erd", pre_up_grad, routed_up_weight, preferred_element_type=float_type
        )
    ).astype(low_type)
    grad_returned = lax.all_to_all(
        from_expert(row_grad, dp_count), "dp", split_axis=0, concat_axis=0, tiled=True
    )
    moe_in_grad = jnp.sum(
        grad_returned.reshape(num_experts * capacity, -1)[places]
        .reshape(tok_count, top_count, -1)
        .astype(float_type),
        axis=1,
    )
    normed_two_grad, weight_grad = lax.psum(
        (shared_in_grad + moe_in_grad, weight_grad_part), "tensor"
    )
    prob_grad = jnp.sum(selector * weight_grad[:, :, None], axis=1)
    logit_grad = (
        router_probs * (prob_grad - jnp.sum(prob_grad * router_probs, axis=-1, keepdims=True))
    ).astype(low_type)
    router_weight_gradient = jnp.dot(normed_two.T, logit_grad, preferred_element_type=float_type)
    normed_two_grad = normed_two_grad + jnp.dot(
        logit_grad, back_router.T, preferred_element_type=float_type
    )
    norm_two_back, feedforward_gain_gradient = rms_back(
        normed_two_grad, mid, recip_two, back_ffn_gain.astype(float_type)
    )
    mid_grad = grad_float + norm_two_back
    mid_low = mid_grad.astype(low_type)
    output_projection_gradient = jnp.dot(attn_flat.T, mid_low, preferred_element_type=float_type)
    heads_grad = by_seq(
        jnp.dot(mid_low, back_output.T, preferred_element_type=float_type)
        .astype(low_type)
        .reshape(tok_count, head_count, DV)
    )
    scale = head_dim ** (-0.5)
    scores = attend_scores(query_seq, key_nope, rope_seq, allowed)
    attn_probs = jnp.exp(scores - log_total)
    probs_low = attn_probs.astype(low_type)
    values_grad = jnp.einsum(
        "shqk,sqhd->skhd", probs_low, heads_grad, preferred_element_type=float_type
    )
    probs_grad = jnp.einsum(
        "sqhd,skhd->shqk", heads_grad, values, preferred_element_type=float_type
    )
    delta = jnp.sum(heads_grad.astype(float_type) * heads_out.astype(float_type), axis=-1)
    delta = jnp.transpose(delta, (0, 2, 1))[..., None]
    score_grad = (attn_probs * (probs_grad - delta) * scale).astype(low_type)
    nope_grad_q = jnp.einsum(
        "shqk,skhd->sqhd", score_grad, key_nope, preferred_element_type=float_type
    )
    rope_grad_q = jnp.einsum(
        "shqk,skd->sqhd", score_grad, rope_seq, preferred_element_type=float_type
    )
    key_nope_grad = jnp.einsum(
        "shqk,sqhd->skhd", score_grad, query_seq[..., :NOPE], preferred_element_type=float_type
    )
    key_rope_grad = jnp.einsum(
        "shqk,sqhd->skd", score_grad, query_seq[..., NOPE:], preferred_element_type=float_type
    )
    query_grad = jnp.concatenate([nope_grad_q, rope_grad_q], axis=-1).reshape(
        tok_count, head_count, head_dim
    )
    query_raw_grad = (
        jnp.concatenate(
            [
                query_grad[..., :NOPE],
                rotate(query_grad[..., NOPE:], cos_tok[:, None], -sin_tok[:, None]),
            ],
            axis=-1,
        )
        .astype(low_type)
        .reshape(tok_count, head_count * head_dim)
    )
    query_projection_gradient = jnp.dot(
        normed_one.T, query_raw_grad, preferred_element_type=float_type
    )
    kv_grad = (
        jnp.concatenate([key_nope_grad, values_grad], axis=-1)
        .astype(low_type)
        .reshape(tok_count, head_count * (NOPE + DV))
    )
    latent_up_gradient = jnp.dot(latent_normed.T, kv_grad, preferred_element_type=float_type)
    normed_one_part = jnp.dot(query_raw_grad, back_query.T, preferred_element_type=float_type)
    latent_part_grad = jnp.dot(kv_grad, back_up.T, preferred_element_type=float_type)
    rope_part_grad = key_rope_grad.reshape(tok_count, ROPE)
    normed_one_grad, latent_normed_grad, rope_key_grad = (
        lax.psum(normed_one_part.astype(jnp.bfloat16), "tensor").astype(jnp.float32),
        lax.psum(latent_part_grad.astype(jnp.bfloat16), "tensor").astype(jnp.float32),
        lax.psum(rope_part_grad.astype(jnp.bfloat16), "tensor").astype(jnp.float32),
    )
    latent_grad, latent_gain_gradient = rms_back(
        latent_normed_grad, latent, recip_latent, back_lgain.astype(float_type)
    )
    rope_pre_grad = rotate(rope_key_grad, cos_tok, -sin_tok)
    down_grad = jnp.concatenate([latent_grad, rope_pre_grad], axis=-1).astype(low_type)
    latent_down_gradient = jnp.dot(normed_one.T, down_grad, preferred_element_type=float_type)
    normed_one_grad = normed_one_grad + jnp.dot(
        down_grad, back_down.T, preferred_element_type=float_type
    )
    norm_one_back, attention_gain_gradient = rms_back(
        normed_one_grad, residual_in, recip_one, back_attn_gain.astype(float_type)
    )
    hidden_input_gradient = mid_grad + norm_one_back
    accumulated_total = tuple(
        (
            lax.psum_scatter(attention_gain_gradient, "dp", scatter_dimension=0, tiled=True),
            lax.psum_scatter(query_projection_gradient, "dp", scatter_dimension=0, tiled=True),
            lax.psum_scatter(latent_down_gradient, "dp", scatter_dimension=0, tiled=True),
            lax.psum_scatter(latent_gain_gradient, "dp", scatter_dimension=0, tiled=True),
            lax.psum_scatter(latent_up_gradient, "dp", scatter_dimension=0, tiled=True),
            lax.psum_scatter(output_projection_gradient, "dp", scatter_dimension=1, tiled=True),
            lax.psum_scatter(feedforward_gain_gradient, "dp", scatter_dimension=0, tiled=True),
            lax.psum_scatter(router_weight_gradient, "dp", scatter_dimension=0, tiled=True),
            lax.psum_scatter(shared_gate_gradient, "dp", scatter_dimension=0, tiled=True),
            lax.psum_scatter(shared_up_gradient, "dp", scatter_dimension=0, tiled=True),
            lax.psum_scatter(shared_down_gradient, "dp", scatter_dimension=1, tiled=True),
        )
    )
    return (
        (output, hidden_input_gradient)
        + accumulated_total
        + (routed_gate_gradient, routed_up_gradient, routed_down_gradient)
    )


def expert_tables(ids, expert, capacity):
    match = jnp.any(ids == expert, axis=-1)
    count = match.astype(jnp.int32)
    place = jnp.where(match, jnp.cumsum(count, axis=-1) - count, capacity)
    slots = jnp.arange(capacity, dtype=jnp.int32)
    return (place[:, None, :] == slots[None, :, None]).astype(jnp.bfloat16)


def gather_rows(table, tokens):
    width = tokens.shape[1]
    blocks = tokens.reshape(table.shape[0], table.shape[2], width)
    rows = jnp.einsum("sct,std->scd", table, blocks, preferred_element_type=jnp.float32)
    return rows.astype(jnp.bfloat16).reshape(-1, width)


def place_rows(table, rows):
    blocks = rows.reshape(table.shape[0], table.shape[1], -1)
    spread = jnp.einsum("sct,scd->std", table, blocks, preferred_element_type=jnp.float32)
    return spread.reshape(-1, spread.shape[-1])


def local_gathered(
    hidden_in,
    segments,
    expert_ids,
    grad_out,
    attn_gain,
    query_proj,
    latent_down,
    latent_gain,
    latent_up,
    output_proj,
    ffn_gain,
    router_weight,
    shared_gate,
    shared_up,
    shared_down,
    routed_gate_weight,
    routed_up_weight,
    routed_down_weight,
):
    float_type = jnp.float32
    low_type = jnp.bfloat16
    tok_count = hidden_in.shape[0]
    width = hidden_in.shape[1]
    seq_count = segments.shape[0]
    seq_len = segments.shape[1]
    top_count = expert_ids.shape[1]
    head_dim = NOPE + ROPE
    dp_count = lax.axis_size("dp")
    my_dp = lax.axis_index("dp")
    local_experts = routed_gate_weight.shape[0]
    num_experts = router_weight.shape[1]
    capacity = 3 * tok_count * top_count // (2 * num_experts)
    d_part = query_proj.shape[0]
    lat_part = latent_up.shape[0]
    hid_slice = shared_gate.shape[1] // dp_count

    small = jnp.concatenate(
        [
            attn_gain,
            ffn_gain,
            latent_gain,
            router_weight.reshape(-1),
            expert_ids.T.reshape(-1).astype(low_type),
        ]
    )
    small_all = lax.all_gather(small, "dp", axis=0, tiled=False)
    cuts = [d_part, d_part, lat_part, d_part * num_experts, tok_count * top_count]
    pieces, at = [], 0
    for size in cuts:
        pieces.append(small_all[:, at : at + size])
        at += size
    full_attn_gain = pieces[0].reshape(-1).astype(float_type)
    full_ffn_gain = pieces[1].reshape(-1).astype(float_type)
    full_lgain = pieces[2].reshape(-1).astype(float_type)
    full_router = pieces[3].reshape(width, num_experts)
    ids_all = jnp.transpose(
        pieces[4].reshape(dp_count, top_count, tok_count).astype(jnp.int32), (0, 2, 1)
    )
    full_query = lax.all_gather(query_proj, "dp", axis=0, tiled=True)
    full_down = lax.all_gather(latent_down, "dp", axis=0, tiled=True)
    full_up = lax.all_gather(latent_up, "dp", axis=0, tiled=True)
    full_output_t = lax.all_gather(output_proj.T, "dp", axis=0, tiled=True)

    shared_send = jnp.concatenate(
        [
            shared_gate.reshape(d_part, dp_count, hid_slice),
            shared_up.reshape(d_part, dp_count, hid_slice),
            shared_down.T.reshape(d_part, dp_count, hid_slice),
        ],
        axis=-1,
    )
    shared_mine = lax.all_to_all(
        jnp.transpose(shared_send, (1, 0, 2)), "dp", split_axis=0, concat_axis=0, tiled=True
    ).reshape(width, 3 * hid_slice)
    gate_up_w = shared_mine[:, : 2 * hid_slice]
    down_w_t = shared_mine[:, 2 * hid_slice :]
    grad_all = lax.all_gather(grad_out, "dp", axis=0, tiled=True)

    def by_seq(array):
        return array.reshape((seq_count, seq_len) + array.shape[1:])

    residual_in = hidden_in.astype(float_type)
    recip_one = rms_recip(residual_in)
    normed_one = (residual_in * recip_one * full_attn_gain).astype(low_type)
    cos_table, sin_table = rope_tables(seq_len, ROPE)
    cos_tok = jnp.tile(cos_table, (seq_count, 1))
    sin_tok = jnp.tile(sin_table, (seq_count, 1))
    head_count = full_query.shape[1] // head_dim
    query_raw = jnp.dot(normed_one, full_query, preferred_element_type=float_type).reshape(
        tok_count, head_count, head_dim
    )
    queries = jnp.concatenate(
        [query_raw[..., :NOPE], rotate(query_raw[..., NOPE:], cos_tok[:, None], sin_tok[:, None])],
        axis=-1,
    ).astype(low_type)
    down_raw = jnp.dot(normed_one, full_down, preferred_element_type=float_type)
    latent = down_raw[:, :LAT]
    recip_latent = rms_recip(latent)
    latent_normed = (latent * recip_latent * full_lgain).astype(low_type)
    key_rope = rotate(down_raw[:, LAT:], cos_tok, sin_tok).astype(low_type)
    keys_values = (
        jnp.dot(latent_normed, full_up, preferred_element_type=float_type)
        .astype(low_type)
        .reshape(tok_count, head_count, NOPE + DV)
    )
    key_nope = by_seq(keys_values[..., :NOPE])
    values = by_seq(keys_values[..., NOPE:])
    query_seq = by_seq(queries)
    rope_seq = by_seq(key_rope)
    allowed = mask_table(segments)
    scores = attend_scores(query_seq, key_nope, rope_seq, allowed)
    highest = jnp.max(scores, axis=-1, keepdims=True)
    log_total = highest + jnp.log(jnp.sum(jnp.exp(scores - highest), axis=-1, keepdims=True))
    attn_probs = jnp.exp(scores - log_total)
    probs_low = attn_probs.astype(low_type)
    heads_out = jnp.einsum(
        "shqk,skhd->sqhd", probs_low, values, preferred_element_type=float_type
    ).astype(low_type)
    attn_flat = heads_out.reshape(tok_count, head_count * DV)
    attn_part = lax.dot_general(
        attn_flat, full_output_t, (((1,), (1,)), ((), ())), preferred_element_type=float_type
    )
    attn_full = lax.psum(attn_part.astype(low_type), "tensor").astype(float_type)
    mid = residual_in + attn_full
    recip_two = rms_recip(mid)
    normed_two = (mid * recip_two * full_ffn_gain).astype(low_type)
    tok_all = lax.all_gather(normed_two, "dp", axis=0, tiled=True)

    logits_all = jnp.dot(tok_all, full_router, preferred_element_type=float_type)
    probs_all = jax.nn.softmax(logits_all, axis=-1)
    router_probs = jax.nn.softmax(
        jnp.dot(normed_two, full_router, preferred_element_type=float_type), axis=-1
    )

    pre_all = jnp.dot(tok_all, gate_up_w, preferred_element_type=float_type)
    shared_pre_up = pre_all[:, hid_slice:]
    shared_act, shared_slope = silu_parts(pre_all[:, :hid_slice])
    shared_hidden = (shared_act * shared_pre_up).astype(low_type)
    shared_act_grad = jnp.dot(grad_all, down_w_t, preferred_element_type=float_type)
    shared_grads = jnp.concatenate(
        [shared_act_grad * shared_pre_up * shared_slope, shared_act_grad * shared_act], axis=-1
    ).astype(low_type)
    ffn_part = lax.dot_general(
        shared_hidden, down_w_t, (((1,), (1,)), ((), ())), preferred_element_type=float_type
    )
    in_grad_part = lax.dot_general(
        shared_grads, gate_up_w, (((1,), (1,)), ((), ())), preferred_element_type=float_type
    )

    expert_columns, routed_grads = [], []
    for index in range(local_experts):
        expert = my_dp * local_experts + index
        gate_w = routed_gate_weight[index]
        up_w = routed_up_weight[index]
        down_w = routed_down_weight[index]
        table = expert_tables(ids_all, expert, capacity)
        token_rows = gather_rows(table, tok_all)
        grad_rows = gather_rows(table, grad_all).astype(float_type)
        column = jnp.sum(
            jnp.where(jnp.arange(num_experts, dtype=jnp.int32) == expert, probs_all, 0.0), axis=-1
        ).reshape(dp_count, 1, tok_count)
        gate_of = jnp.sum(table.astype(float_type) * column, axis=-1).reshape(-1, 1)
        pre_gate = jnp.dot(token_rows, gate_w, preferred_element_type=float_type)
        pre_up = jnp.dot(token_rows, up_w, preferred_element_type=float_type)
        expert_act, expert_slope = silu_parts(pre_gate)
        expert_hidden = (expert_act * pre_up).astype(low_type)
        expert_result = jnp.dot(expert_hidden, down_w, preferred_element_type=float_type).astype(
            low_type
        )
        result_float = expert_result.astype(float_type)
        weight_rows = jnp.sum(grad_rows * result_float, axis=-1).reshape(dp_count, capacity, 1)
        expert_columns.append(jnp.sum(table.astype(float_type) * weight_rows, axis=1))
        ffn_part = ffn_part + place_rows(table, (gate_of * result_float).astype(low_type))
        slot_grad = (gate_of * grad_rows).astype(low_type)
        hidden_grad = lax.dot_general(
            slot_grad, down_w, (((1,), (1,)), ((), ())), preferred_element_type=float_type
        )
        pre_gate_grad = (hidden_grad * pre_up * expert_slope).astype(low_type)
        pre_up_grad = (hidden_grad * expert_act).astype(low_type)
        row_grad = lax.dot_general(
            pre_gate_grad, gate_w, (((1,), (1,)), ((), ())), preferred_element_type=float_type
        )
        row_grad = row_grad + lax.dot_general(
            pre_up_grad, up_w, (((1,), (1,)), ((), ())), preferred_element_type=float_type
        )
        in_grad_part = in_grad_part + place_rows(table, row_grad.astype(low_type))
        routed_grads.append(
            (
                jnp.dot(token_rows.T, pre_gate_grad, preferred_element_type=float_type),
                jnp.dot(token_rows.T, pre_up_grad, preferred_element_type=float_type),
                jnp.dot(expert_hidden.T, slot_grad, preferred_element_type=float_type),
            )
        )
    routed_out = tuple(jnp.stack(parts) for parts in zip(*routed_grads))

    prob_send = jnp.stack(expert_columns, axis=1)
    prob_part = jnp.transpose(
        lax.all_to_all(prob_send, "dp", split_axis=0, concat_axis=0, tiled=True).reshape(
            num_experts, tok_count
        )
    )
    prob_grad = lax.psum(prob_part, "tensor")
    in_grad = lax.psum_scatter(
        in_grad_part.astype(low_type), "dp", scatter_dimension=0, tiled=True
    )
    normed_two_grad = lax.psum(in_grad, "tensor").astype(float_type)
    ffn_sum = lax.psum_scatter(ffn_part.astype(low_type), "dp", scatter_dimension=0, tiled=True)
    ffn_full = lax.psum(ffn_sum, "tensor").astype(float_type)
    output = (mid + ffn_full).astype(low_type)

    shared_gate_up_grad = jnp.dot(tok_all.T, shared_grads, preferred_element_type=float_type)
    shared_down_grad_t = jnp.dot(grad_all.T, shared_hidden, preferred_element_type=float_type)
    shared_back = jnp.concatenate([shared_gate_up_grad, shared_down_grad_t], axis=-1).astype(
        low_type
    )
    shared_back = lax.all_to_all(
        shared_back.reshape(dp_count, d_part, 3 * hid_slice),
        "dp",
        split_axis=0,
        concat_axis=0,
        tiled=True,
    )
    shared_back = jnp.transpose(shared_back, (1, 0, 2)).astype(float_type)
    shared_gate_gradient = shared_back[..., :hid_slice].reshape(d_part, -1)
    shared_up_gradient = shared_back[..., hid_slice : 2 * hid_slice].reshape(d_part, -1)
    shared_down_gradient = shared_back[..., 2 * hid_slice :].reshape(d_part, -1).T

    grad_float = grad_out.astype(float_type)
    logit_grad = (
        router_probs * (prob_grad - jnp.sum(prob_grad * router_probs, axis=-1, keepdims=True))
    ).astype(low_type)
    router_weight_gradient = jnp.dot(normed_two.T, logit_grad, preferred_element_type=float_type)
    normed_two_grad = normed_two_grad + jnp.dot(
        logit_grad, full_router.T, preferred_element_type=float_type
    )
    norm_two_back, feedforward_gain_gradient = rms_back(
        normed_two_grad, mid, recip_two, full_ffn_gain
    )
    mid_grad = grad_float + norm_two_back
    mid_low = mid_grad.astype(low_type)
    output_projection_gradient_t = jnp.dot(
        mid_low.T, attn_flat, preferred_element_type=float_type
    )
    heads_grad = by_seq(
        jnp.dot(mid_low, full_output_t, preferred_element_type=float_type)
        .astype(low_type)
        .reshape(tok_count, head_count, DV)
    )
    scale = head_dim ** (-0.5)
    values_grad = jnp.einsum(
        "shqk,sqhd->skhd", probs_low, heads_grad, preferred_element_type=float_type
    )
    probs_grad = jnp.einsum(
        "sqhd,skhd->shqk", heads_grad, values, preferred_element_type=float_type
    )
    delta = jnp.sum(heads_grad.astype(float_type) * heads_out.astype(float_type), axis=-1)
    delta = jnp.transpose(delta, (0, 2, 1))[..., None]
    score_grad = (attn_probs * (probs_grad - delta) * scale).astype(low_type)
    nope_grad_q = jnp.einsum(
        "shqk,skhd->sqhd", score_grad, key_nope, preferred_element_type=float_type
    )
    rope_grad_q = jnp.einsum(
        "shqk,skd->sqhd", score_grad, rope_seq, preferred_element_type=float_type
    )
    key_nope_grad = jnp.einsum(
        "shqk,sqhd->skhd", score_grad, query_seq[..., :NOPE], preferred_element_type=float_type
    )
    key_rope_grad = jnp.einsum(
        "shqk,sqhd->skd", score_grad, query_seq[..., NOPE:], preferred_element_type=float_type
    )
    query_grad = jnp.concatenate([nope_grad_q, rope_grad_q], axis=-1).reshape(
        tok_count, head_count, head_dim
    )
    query_raw_grad = (
        jnp.concatenate(
            [
                query_grad[..., :NOPE],
                rotate(query_grad[..., NOPE:], cos_tok[:, None], -sin_tok[:, None]),
            ],
            axis=-1,
        )
        .astype(low_type)
        .reshape(tok_count, head_count * head_dim)
    )
    query_projection_gradient = jnp.dot(
        normed_one.T, query_raw_grad, preferred_element_type=float_type
    )
    kv_grad = (
        jnp.concatenate([key_nope_grad, values_grad], axis=-1)
        .astype(low_type)
        .reshape(tok_count, head_count * (NOPE + DV))
    )
    latent_up_gradient = jnp.dot(latent_normed.T, kv_grad, preferred_element_type=float_type)
    normed_one_part = lax.dot_general(
        query_raw_grad, full_query, (((1,), (1,)), ((), ())), preferred_element_type=float_type
    )
    latent_part_grad = lax.dot_general(
        kv_grad, full_up, (((1,), (1,)), ((), ())), preferred_element_type=float_type
    )
    rope_part_grad = key_rope_grad.reshape(tok_count, ROPE)
    parts = jnp.concatenate(
        [normed_one_part, latent_part_grad, rope_part_grad], axis=-1
    ).astype(low_type)
    sums = lax.psum(parts, "tensor").astype(float_type)
    normed_one_grad = sums[:, :width]
    latent_normed_grad = sums[:, width : width + LAT]
    rope_key_grad = sums[:, width + LAT :]
    latent_grad, latent_gain_gradient = rms_back(
        latent_normed_grad, latent, recip_latent, full_lgain
    )
    rope_pre_grad = rotate(rope_key_grad, cos_tok, -sin_tok)
    down_grad = jnp.concatenate([latent_grad, rope_pre_grad], axis=-1).astype(low_type)
    latent_down_gradient = jnp.dot(normed_one.T, down_grad, preferred_element_type=float_type)
    normed_one_grad = normed_one_grad + lax.dot_general(
        down_grad, full_down, (((1,), (1,)), ((), ())), preferred_element_type=float_type
    )
    norm_one_back, attention_gain_gradient = rms_back(
        normed_one_grad, residual_in, recip_one, full_attn_gain
    )
    hidden_input_gradient = mid_grad + norm_one_back

    def scatter(array):
        return lax.psum_scatter(
            array.astype(low_type), "dp", scatter_dimension=0, tiled=True
        ).astype(float_type)

    small_grads = jnp.concatenate(
        [
            attention_gain_gradient.reshape(dp_count, -1),
            feedforward_gain_gradient.reshape(dp_count, -1),
            latent_gain_gradient.reshape(dp_count, -1),
            router_weight_gradient.reshape(dp_count, -1),
        ],
        axis=-1,
    )
    small_sums = lax.psum_scatter(small_grads, "dp", scatter_dimension=0, tiled=True).reshape(-1)
    one, two, three = d_part, 2 * d_part, 2 * d_part + lat_part
    return (
        output,
        hidden_input_gradient,
        small_sums[:one],
        scatter(query_projection_gradient),
        scatter(latent_down_gradient),
        small_sums[two:three],
        scatter(latent_up_gradient),
        scatter(output_projection_gradient_t).T,
        small_sums[one:two],
        small_sums[three:].reshape(d_part, num_experts),
        shared_gate_gradient,
        shared_up_gradient,
        shared_down_gradient,
    ) + routed_out


def local(*arrays):
    tok_count, top_count = arrays[0].shape[0], arrays[2].shape[1]
    gathered_rows = lax.axis_size("dp") * tok_count
    slot_rows = 3 * tok_count * top_count // 2
    if gathered_rows <= 2 * slot_rows:
        return local_gathered(*arrays)
    return local_exchanged(*arrays)


def solution(mesh):
    return jax.shard_map(
        local,
        mesh=mesh,
        in_specs=(
            P("dp", None),
            P("dp", None),
            P("dp", None),
            P("dp", None),
            P("dp"),
            P("dp", "tensor"),
            P("dp", None),
            P("dp"),
            P("dp", "tensor"),
            P("tensor", "dp"),
            P("dp"),
            P("dp", None),
            P("dp", "tensor"),
            P("dp", "tensor"),
            P("tensor", "dp"),
            P("dp", None, "tensor"),
            P("dp", None, "tensor"),
            P("dp", "tensor", None),
        ),
        out_specs=(
            P("dp", None),
            P("dp", None),
            P("dp"),
            P("dp", "tensor"),
            P("dp", None),
            P("dp"),
            P("dp", "tensor"),
            P("tensor", "dp"),
            P("dp"),
            P("dp", None),
            P("dp", "tensor"),
            P("dp", "tensor"),
            P("tensor", "dp"),
            P("dp", None, "tensor"),
            P("dp", None, "tensor"),
            P("dp", "tensor", None),
        ),
        check_vma=False,
    )
```

```python
import jax
import jax.numpy as jnp
from jax import lax
from jax.experimental import pallas as pl
from jax.experimental.pallas import tpu as pltpu
from jax.sharding import PartitionSpec as P

NOPE = 128
ROPE = 64
DV = 128
LAT = 512


EPS = 1e-06
ROPE_BASE = 10000.0
NEG_FILL = -1e30


def rope_tables(length, width):
    half_width = width // 2
    frequency = ROPE_BASE ** (-(jnp.arange(half_width, dtype=jnp.float32) * (2.0 / width)))
    angles = jnp.arange(length, dtype=jnp.float32)[:, None] * frequency[None, :]
    angles = jnp.concatenate([angles, angles], axis=1)
    return (jnp.cos(angles), jnp.sin(angles))


def rotate(values, cos_table, sin_table):
    half_width = values.shape[-1] // 2
    turned = jnp.concatenate([-values[..., half_width:], values[..., :half_width]], axis=-1)
    return values * cos_table + turned * sin_table


def rms_recip(values):
    return lax.rsqrt(jnp.mean(values * values, axis=-1, keepdims=True) + EPS)


def rms_back(grad_normed, values, recip, gain):
    hat_values = values * recip
    scaled = grad_normed * gain
    grad_in = recip * (scaled - hat_values * jnp.mean(scaled * hat_values, axis=-1, keepdims=True))
    grad_gain = jnp.sum(grad_normed * hat_values, axis=0)
    return (grad_in, grad_gain)


def silu_parts(pre_act):
    sigmoid_val = jax.nn.sigmoid(pre_act)
    return (pre_act * sigmoid_val, sigmoid_val * (1.0 + pre_act * (1.0 - sigmoid_val)))


def mask_table(segments):
    places = jnp.arange(segments.shape[1], dtype=jnp.int32)
    same_doc = segments[:, :, None] == segments[:, None, :]
    return same_doc & (places[None, None, :] <= places[None, :, None])


def attend_scores(query_all, key_nope, key_rope, allowed):
    nope_width = key_nope.shape[-1]
    scale = query_all.shape[-1] ** (-0.5)
    scores = jnp.einsum(
        "sqhd,skhd->shqk", query_all[..., :nope_width], key_nope, preferred_element_type=jnp.float32
    )
    scores = scores + jnp.einsum(
        "sqhd,skd->shqk", query_all[..., nope_width:], key_rope, preferred_element_type=jnp.float32
    )
    return jnp.where(allowed[:, None], scores * scale, NEG_FILL)


def slot_positions(chosen, experts):
    matches = (
        (chosen[:, :, None] == jnp.arange(experts, dtype=jnp.int32))
        .astype(jnp.int32)
        .reshape(-1, experts)
    )
    earlier = jnp.cumsum(matches, axis=0) - matches
    return jnp.sum(earlier * matches, axis=1).reshape(chosen.shape)


def to_expert(arrived, sources, local_count):
    capacity = arrived.shape[1]
    feature_width = arrived.shape[2]
    grouped = arrived.reshape(sources, local_count, capacity, feature_width)
    return jnp.transpose(grouped, (1, 0, 2, 3)).reshape(
        local_count, sources * capacity, feature_width
    )


def from_expert(expert_rows, sources):
    local_count = expert_rows.shape[0]
    capacity = expert_rows.shape[1] // sources
    feature_width = expert_rows.shape[2]
    grouped = expert_rows.reshape(local_count, sources, capacity, feature_width)
    return jnp.transpose(grouped, (1, 0, 2, 3)).reshape(
        sources * local_count, capacity, feature_width
    )


def local_exchanged(
    hidden_in,
    segments,
    expert_ids,
    grad_out,
    attn_gain,
    query_proj,
    latent_down,
    latent_gain,
    latent_up,
    output_proj,
    ffn_gain,
    router_weight,
    shared_gate,
    shared_up,
    shared_down,
    routed_gate_weight,
    routed_up_weight,
    routed_down_weight,
):
    float_type = jnp.float32
    low_type = jnp.bfloat16
    tok_count = hidden_in.shape[0]
    seq_count = segments.shape[0]
    seq_len = segments.shape[1]
    top_count = expert_ids.shape[1]
    head_dim = NOPE + ROPE
    dp_count = lax.axis_size("dp")
    local_experts = routed_gate_weight.shape[0]
    dense_weights = (
        attn_gain,
        query_proj,
        latent_down,
        latent_gain,
        latent_up,
        output_proj,
        ffn_gain,
        router_weight,
        shared_gate,
        shared_up,
        shared_down,
    )
    gathered = (
        lax.all_gather(dense_weights[0], "dp", axis=0, tiled=True),
        lax.all_gather(dense_weights[1], "dp", axis=0, tiled=True),
        lax.all_gather(dense_weights[2], "dp", axis=0, tiled=True),
        lax.all_gather(dense_weights[3], "dp", axis=0, tiled=True),
        lax.all_gather(dense_weights[4], "dp", axis=0, tiled=True),
        lax.all_gather(dense_weights[5], "dp", axis=1, tiled=True),
        lax.all_gather(dense_weights[6], "dp", axis=0, tiled=True),
        lax.all_gather(dense_weights[7], "dp", axis=0, tiled=True),
        lax.all_gather(dense_weights[8], "dp", axis=0, tiled=True),
        lax.all_gather(dense_weights[9], "dp", axis=0, tiled=True),
        lax.all_gather(dense_weights[10], "dp", axis=1, tiled=True),
    )
    (
        full_attn_gain,
        full_query,
        full_down,
        full_lgain,
        full_up,
        full_output,
        full_ffn_gain,
        full_router,
        full_sgate,
        full_sup,
        full_sdown,
    ) = gathered
    num_experts = full_router.shape[1]
    capacity = 3 * tok_count * top_count // (2 * num_experts)
    head_count = full_query.shape[1] // head_dim

    def by_seq(array):
        return array.reshape((seq_count, seq_len) + array.shape[1:])

    residual_in = hidden_in.astype(float_type)
    recip_one = rms_recip(residual_in)
    normed_one = (residual_in * recip_one * full_attn_gain.astype(float_type)).astype(low_type)
    cos_table, sin_table = rope_tables(seq_len, ROPE)
    cos_tok = jnp.tile(cos_table, (seq_count, 1))
    sin_tok = jnp.tile(sin_table, (seq_count, 1))
    query_raw = jnp.dot(normed_one, full_query, preferred_element_type=float_type).reshape(
        tok_count, head_count, head_dim
    )
    queries = jnp.concatenate(
        [query_raw[..., :NOPE], rotate(query_raw[..., NOPE:], cos_tok[:, None], sin_tok[:, None])],
        axis=-1,
    ).astype(low_type)
    down_raw = jnp.dot(normed_one, full_down, preferred_element_type=float_type)
    latent = down_raw[:, :LAT]
    recip_latent = rms_recip(latent)
    latent_normed = (latent * recip_latent * full_lgain.astype(float_type)).astype(low_type)
    key_rope = rotate(down_raw[:, LAT:], cos_tok, sin_tok).astype(low_type)
    keys_values = (
        jnp.dot(latent_normed, full_up, preferred_element_type=float_type)
        .astype(low_type)
        .reshape(tok_count, head_count, NOPE + DV)
    )
    key_nope = by_seq(keys_values[..., :NOPE])
    values = by_seq(keys_values[..., NOPE:])
    query_seq = by_seq(queries)
    rope_seq = by_seq(key_rope)
    allowed = mask_table(segments)
    scores = attend_scores(query_seq, key_nope, rope_seq, allowed)
    highest = jnp.max(scores, axis=-1, keepdims=True)
    log_total = highest + jnp.log(jnp.sum(jnp.exp(scores - highest), axis=-1, keepdims=True))
    attn_probs = jnp.exp(scores - log_total).astype(low_type)
    heads_out = jnp.einsum(
        "shqk,skhd->sqhd", attn_probs, values, preferred_element_type=float_type
    ).astype(low_type)
    attn_flat = heads_out.reshape(tok_count, head_count * DV)
    attn_part = jnp.dot(attn_flat, full_output, preferred_element_type=float_type)
    attn_full = lax.psum(attn_part, "tensor")
    mid = residual_in + attn_full
    recip_two = rms_recip(mid)
    normed_two = (mid * recip_two * full_ffn_gain.astype(float_type)).astype(low_type)
    logits = jnp.dot(normed_two, full_router, preferred_element_type=float_type)
    router_probs = jax.nn.softmax(logits, axis=-1)
    selector = (expert_ids[:, :, None] == jnp.arange(num_experts, dtype=jnp.int32)).astype(
        float_type
    )
    gate_weight = jnp.sum(selector * router_probs[:, None, :], axis=-1)
    shared_pre_gate = jnp.dot(normed_two, full_sgate, preferred_element_type=float_type)
    shared_pre_up = jnp.dot(normed_two, full_sup, preferred_element_type=float_type)
    shared_act, shared_slope = silu_parts(shared_pre_gate)
    shared_hidden = (shared_act * shared_pre_up).astype(low_type)
    shared_part = jnp.dot(shared_hidden, full_sdown, preferred_element_type=float_type)
    slots = slot_positions(expert_ids, num_experts)
    place_grid = expert_ids * capacity + slots
    places = place_grid.reshape(-1)
    place_rows = jnp.arange(num_experts * capacity, dtype=jnp.int32)
    dispatch_table = jnp.sum(
        (place_grid[None, :, :] == place_rows[:, None, None]).astype(low_type), axis=-1
    )
    send_rows = (
        jnp.dot(dispatch_table, normed_two, preferred_element_type=float_type)
        .astype(low_type)
        .reshape(num_experts, capacity, -1)
    )
    arrived = lax.all_to_all(send_rows, "dp", split_axis=0, concat_axis=0, tiled=True)
    expert_rows = to_expert(arrived, dp_count, local_experts)
    pre_gate = jnp.einsum(
        "erd,edf->erf", expert_rows, routed_gate_weight, preferred_element_type=float_type
    )
    pre_up = jnp.einsum(
        "erd,edf->erf", expert_rows, routed_up_weight, preferred_element_type=float_type
    )
    expert_act, expert_slope = silu_parts(pre_gate)
    expert_hidden = (expert_act * pre_up).astype(low_type)
    expert_result = jnp.einsum(
        "erf,efd->erd", expert_hidden, routed_down_weight, preferred_element_type=float_type
    ).astype(low_type)
    returned = lax.all_to_all(
        from_expert(expert_result, dp_count), "dp", split_axis=0, concat_axis=0, tiled=True
    )
    picked = (
        returned.reshape(num_experts * capacity, -1)[places]
        .reshape(tok_count, top_count, -1)
        .astype(float_type)
    )
    moe_part = jnp.sum(gate_weight[:, :, None] * picked, axis=1)
    ffn_full = lax.psum((moe_part + shared_part).astype(jnp.bfloat16), "tensor").astype(jnp.float32)
    output = (mid + ffn_full).astype(low_type)
    back_weights = (
        lax.all_gather(dense_weights[0], "dp", axis=0, tiled=True),
        lax.all_gather(dense_weights[1], "dp", axis=0, tiled=True),
        lax.all_gather(dense_weights[2], "dp", axis=0, tiled=True),
        lax.all_gather(dense_weights[3], "dp", axis=0, tiled=True),
        lax.all_gather(dense_weights[4], "dp", axis=0, tiled=True),
        lax.all_gather(dense_weights[5], "dp", axis=1, tiled=True),
        lax.all_gather(dense_weights[6], "dp", axis=0, tiled=True),
        lax.all_gather(dense_weights[7], "dp", axis=0, tiled=True),
        lax.all_gather(dense_weights[8], "dp", axis=0, tiled=True),
        lax.all_gather(dense_weights[9], "dp", axis=0, tiled=True),
        lax.all_gather(dense_weights[10], "dp", axis=1, tiled=True),
    )
    (
        back_attn_gain,
        back_query,
        back_down,
        back_lgain,
        back_up,
        back_output,
        back_ffn_gain,
        back_router,
        back_sgate,
        back_sup,
        back_sdown,
    ) = back_weights
    grad_float = grad_out.astype(float_type)
    shared_act_grad = jnp.dot(grad_out, back_sdown.T, preferred_element_type=float_type)
    shared_gate_grad = (shared_act_grad * shared_pre_up * shared_slope).astype(low_type)
    shared_up_grad = (shared_act_grad * shared_act).astype(low_type)
    shared_down_gradient = jnp.dot(shared_hidden.T, grad_out, preferred_element_type=float_type)
    shared_gate_gradient = jnp.dot(
        normed_two.T, shared_gate_grad, preferred_element_type=float_type
    )
    shared_up_gradient = jnp.dot(normed_two.T, shared_up_grad, preferred_element_type=float_type)
    shared_in_grad = jnp.dot(shared_gate_grad, back_sgate.T, preferred_element_type=float_type)
    shared_in_grad = shared_in_grad + jnp.dot(
        shared_up_grad, back_sup.T, preferred_element_type=float_type
    )
    weight_grad_part = jnp.sum(grad_float[:, None, :] * picked, axis=-1)
    slot_grad = (
        (gate_weight[:, :, None] * grad_float[:, None, :])
        .astype(low_type)
        .reshape(tok_count * top_count, -1)
    )
    grad_send = (
        jnp.zeros((num_experts * capacity, slot_grad.shape[1]), low_type)
        .at[places]
        .set(slot_grad)
        .reshape(num_experts, capacity, -1)
    )
    grad_arrived = to_expert(
        lax.all_to_all(grad_send, "dp", split_axis=0, concat_axis=0, tiled=True),
        dp_count,
        local_experts,
    )
    hidden_grad = jnp.einsum(
        "erd,efd->erf", grad_arrived, routed_down_weight, preferred_element_type=float_type
    )
    pre_gate_grad = (hidden_grad * pre_up * expert_slope).astype(low_type)
    pre_up_grad = (hidden_grad * expert_act).astype(low_type)
    routed_down_gradient = jnp.einsum(
        "erf,erd->efd", expert_hidden, grad_arrived, preferred_element_type=float_type
    )
    routed_gate_gradient = jnp.einsum(
        "erd,erf->edf", expert_rows, pre_gate_grad, preferred_element_type=float_type
    )
    routed_up_gradient = jnp.einsum(
        "erd,erf->edf", expert_rows, pre_up_grad, preferred_element_type=float_type
    )
    row_grad = jnp.einsum(
        "erf,edf->erd", pre_gate_grad, routed_gate_weight, preferred_element_type=float_type
    )
    row_grad = (
        row_grad
        + jnp.einsum(
            "erf,edf->erd", pre_up_grad, routed_up_weight, preferred_element_type=float_type
        )
    ).astype(low_type)
    grad_returned = lax.all_to_all(
        from_expert(row_grad, dp_count), "dp", split_axis=0, concat_axis=0, tiled=True
    )
    moe_in_grad = jnp.sum(
        grad_returned.reshape(num_experts * capacity, -1)[places]
        .reshape(tok_count, top_count, -1)
        .astype(float_type),
        axis=1,
    )
    normed_two_grad, weight_grad = lax.psum(
        (shared_in_grad + moe_in_grad, weight_grad_part), "tensor"
    )
    prob_grad = jnp.sum(selector * weight_grad[:, :, None], axis=1)
    logit_grad = (
        router_probs * (prob_grad - jnp.sum(prob_grad * router_probs, axis=-1, keepdims=True))
    ).astype(low_type)
    router_weight_gradient = jnp.dot(normed_two.T, logit_grad, preferred_element_type=float_type)
    normed_two_grad = normed_two_grad + jnp.dot(
        logit_grad, back_router.T, preferred_element_type=float_type
    )
    norm_two_back, feedforward_gain_gradient = rms_back(
        normed_two_grad, mid, recip_two, back_ffn_gain.astype(float_type)
    )
    mid_grad = grad_float + norm_two_back
    mid_low = mid_grad.astype(low_type)
    output_projection_gradient = jnp.dot(attn_flat.T, mid_low, preferred_element_type=float_type)
    heads_grad = by_seq(
        jnp.dot(mid_low, back_output.T, preferred_element_type=float_type)
        .astype(low_type)
        .reshape(tok_count, head_count, DV)
    )
    scale = head_dim ** (-0.5)
    scores = attend_scores(query_seq, key_nope, rope_seq, allowed)
    attn_probs = jnp.exp(scores - log_total)
    probs_low = attn_probs.astype(low_type)
    values_grad = jnp.einsum(
        "shqk,sqhd->skhd", probs_low, heads_grad, preferred_element_type=float_type
    )
    probs_grad = jnp.einsum(
        "sqhd,skhd->shqk", heads_grad, values, preferred_element_type=float_type
    )
    delta = jnp.sum(heads_grad.astype(float_type) * heads_out.astype(float_type), axis=-1)
    delta = jnp.transpose(delta, (0, 2, 1))[..., None]
    score_grad = (attn_probs * (probs_grad - delta) * scale).astype(low_type)
    nope_grad_q = jnp.einsum(
        "shqk,skhd->sqhd", score_grad, key_nope, preferred_element_type=float_type
    )
    rope_grad_q = jnp.einsum(
        "shqk,skd->sqhd", score_grad, rope_seq, preferred_element_type=float_type
    )
    key_nope_grad = jnp.einsum(
        "shqk,sqhd->skhd", score_grad, query_seq[..., :NOPE], preferred_element_type=float_type
    )
    key_rope_grad = jnp.einsum(
        "shqk,sqhd->skd", score_grad, query_seq[..., NOPE:], preferred_element_type=float_type
    )
    query_grad = jnp.concatenate([nope_grad_q, rope_grad_q], axis=-1).reshape(
        tok_count, head_count, head_dim
    )
    query_raw_grad = (
        jnp.concatenate(
            [
                query_grad[..., :NOPE],
                rotate(query_grad[..., NOPE:], cos_tok[:, None], -sin_tok[:, None]),
            ],
            axis=-1,
        )
        .astype(low_type)
        .reshape(tok_count, head_count * head_dim)
    )
    query_projection_gradient = jnp.dot(
        normed_one.T, query_raw_grad, preferred_element_type=float_type
    )
    kv_grad = (
        jnp.concatenate([key_nope_grad, values_grad], axis=-1)
        .astype(low_type)
        .reshape(tok_count, head_count * (NOPE + DV))
    )
    latent_up_gradient = jnp.dot(latent_normed.T, kv_grad, preferred_element_type=float_type)
    normed_one_part = jnp.dot(query_raw_grad, back_query.T, preferred_element_type=float_type)
    latent_part_grad = jnp.dot(kv_grad, back_up.T, preferred_element_type=float_type)
    rope_part_grad = key_rope_grad.reshape(tok_count, ROPE)
    normed_one_grad, latent_normed_grad, rope_key_grad = (
        lax.psum(normed_one_part.astype(jnp.bfloat16), "tensor").astype(jnp.float32),
        lax.psum(latent_part_grad.astype(jnp.bfloat16), "tensor").astype(jnp.float32),
        lax.psum(rope_part_grad.astype(jnp.bfloat16), "tensor").astype(jnp.float32),
    )
    latent_grad, latent_gain_gradient = rms_back(
        latent_normed_grad, latent, recip_latent, back_lgain.astype(float_type)
    )
    rope_pre_grad = rotate(rope_key_grad, cos_tok, -sin_tok)
    down_grad = jnp.concatenate([latent_grad, rope_pre_grad], axis=-1).astype(low_type)
    latent_down_gradient = jnp.dot(normed_one.T, down_grad, preferred_element_type=float_type)
    normed_one_grad = normed_one_grad + jnp.dot(
        down_grad, back_down.T, preferred_element_type=float_type
    )
    norm_one_back, attention_gain_gradient = rms_back(
        normed_one_grad, residual_in, recip_one, back_attn_gain.astype(float_type)
    )
    hidden_input_gradient = mid_grad + norm_one_back
    accumulated_total = tuple(
        (
            lax.psum_scatter(attention_gain_gradient, "dp", scatter_dimension=0, tiled=True),
            lax.psum_scatter(query_projection_gradient, "dp", scatter_dimension=0, tiled=True),
            lax.psum_scatter(latent_down_gradient, "dp", scatter_dimension=0, tiled=True),
            lax.psum_scatter(latent_gain_gradient, "dp", scatter_dimension=0, tiled=True),
            lax.psum_scatter(latent_up_gradient, "dp", scatter_dimension=0, tiled=True),
            lax.psum_scatter(output_projection_gradient, "dp", scatter_dimension=1, tiled=True),
            lax.psum_scatter(feedforward_gain_gradient, "dp", scatter_dimension=0, tiled=True),
            lax.psum_scatter(router_weight_gradient, "dp", scatter_dimension=0, tiled=True),
            lax.psum_scatter(shared_gate_gradient, "dp", scatter_dimension=0, tiled=True),
            lax.psum_scatter(shared_up_gradient, "dp", scatter_dimension=0, tiled=True),
            lax.psum_scatter(shared_down_gradient, "dp", scatter_dimension=1, tiled=True),
        )
    )
    return (
        (output, hidden_input_gradient)
        + accumulated_total
        + (routed_gate_gradient, routed_up_gradient, routed_down_gradient)
    )


def slot_of_token(ids, expert, capacity):
    match = jnp.any(ids == expert, axis=-1)
    count = match.astype(jnp.int32)
    return jnp.where(match, jnp.cumsum(count, axis=-1) - count, capacity)


def pick_kernel(place_ref, *refs):
    rows_ref = refs[-1]
    shape = (rows_ref.shape[0], place_ref.shape[2])
    chosen = (lax.broadcasted_iota(jnp.int32, shape, 0) == place_ref[0]).astype(jnp.bfloat16)
    at = 0
    for tokens_ref in refs[:-1]:
        end = at + tokens_ref.shape[1]
        rows_ref[:, at:end] = jnp.dot(
            chosen, tokens_ref[...], preferred_element_type=jnp.float32
        ).astype(jnp.bfloat16)
        at = end


def pick_rows(place, pieces, capacity):
    sources, tok_count = place.shape
    width = sum(piece.shape[1] for piece in pieces)
    token_specs = [
        pl.BlockSpec((tok_count, piece.shape[1]), lambda s: (s, 0)) for piece in pieces
    ]
    return pl.pallas_call(
        pick_kernel,
        grid=(sources,),
        in_specs=[pl.BlockSpec((1, 1, tok_count), lambda s: (s, 0, 0))] + token_specs,
        out_specs=pl.BlockSpec((capacity, width), lambda s: (s, 0)),
        out_shape=jax.ShapeDtypeStruct((sources * capacity, width), jnp.bfloat16),
        cost_estimate=pl.CostEstimate(
            flops=2 * sources * capacity * tok_count * width,
            bytes_accessed=2 * sources * (capacity + tok_count) * width,
            transcendentals=0,
        ),
    )(place[:, None, :], *pieces)


def spread_kernel(place_ref, rows_ref, scale_ref, left_ref, right_ref, *out_refs):
    shape = (place_ref.shape[0], rows_ref.shape[0])
    chosen = lax.broadcasted_iota(jnp.int32, shape, 1) == place_ref[...]
    rows = (rows_ref[...].astype(jnp.float32) * scale_ref[...]).astype(jnp.bfloat16)
    total = jnp.dot(chosen.astype(jnp.bfloat16), rows, preferred_element_type=jnp.float32)
    total = total + jnp.dot(left_ref[...], right_ref[...], preferred_element_type=jnp.float32)
    at = 0
    for out_ref in out_refs:
        end = at + out_ref.shape[0]
        out_ref[...] = total[at:end].astype(jnp.bfloat16)
        at = end


def spread_rows(place, rows, scale, left, right, parts):
    sources, tok_count = place.shape
    capacity = rows.shape[0] // sources
    depth, width = right.shape
    size = tok_count // parts
    return pl.pallas_call(
        spread_kernel,
        grid=(sources,),
        in_specs=[
            pl.BlockSpec((tok_count, 1), lambda s: (s, 0)),
            pl.BlockSpec((capacity, width), lambda s: (s, 0)),
            pl.BlockSpec((capacity, 1), lambda s: (s, 0)),
            pl.BlockSpec((tok_count, depth), lambda s: (s, 0)),
            pl.BlockSpec((depth, width), lambda s: (0, 0)),
        ],
        out_specs=[pl.BlockSpec((size, width), lambda s: (s, 0))] * parts,
        out_shape=[jax.ShapeDtypeStruct((sources * size, width), jnp.bfloat16)] * parts,
        cost_estimate=pl.CostEstimate(
            flops=2 * sources * tok_count * width * (capacity + depth),
            bytes_accessed=2 * sources * (capacity + tok_count) * width,
            transcendentals=0,
        ),
    )(place.reshape(-1, 1), rows, scale, left, right)


def pack_kernel(normed_ref, query_ref, down_ref, up_ref, extra_ref, out_ref):
    contract = (((0,), (0,)), ((), ()))
    normed = normed_ref[...]
    query_width = query_ref.shape[1]
    lat_part, up_width = up_ref.shape
    up_cols = lat_part * up_width // out_ref.shape[0]
    out_ref[:, :query_width] = lax.dot_general(
        normed, query_ref[...], contract, preferred_element_type=jnp.float32
    ).astype(jnp.bfloat16)
    for index in range(up_width // up_cols):
        out_ref[index * lat_part : (index + 1) * lat_part, query_width : query_width + up_cols] = (
            up_ref[:, index * up_cols : (index + 1) * up_cols]
        )
    down = lax.dot_general(normed, down_ref[...], contract, preferred_element_type=jnp.float32)
    out_ref[:, query_width + up_cols :] = (down + extra_ref[...].astype(jnp.float32)).astype(
        jnp.bfloat16
    )


def pack_grads(normed, query_grad, down_grad, up_grad, extra, dp_count):
    tok_count, width = normed.shape
    d_part = width // dp_count
    lat_part = up_grad.shape[0] // dp_count
    up_cols = lat_part * up_grad.shape[1] // d_part
    total = query_grad.shape[1] + up_cols + down_grad.shape[1]
    return pl.pallas_call(
        pack_kernel,
        grid=(dp_count,),
        in_specs=[
            pl.BlockSpec((tok_count, d_part), lambda d: (0, d)),
            pl.BlockSpec(query_grad.shape, lambda d: (0, 0)),
            pl.BlockSpec(down_grad.shape, lambda d: (0, 0)),
            pl.BlockSpec((lat_part, up_grad.shape[1]), lambda d: (d, 0)),
            pl.BlockSpec((d_part, extra.shape[1]), lambda d: (d, 0)),
        ],
        out_specs=pl.BlockSpec((d_part, total), lambda d: (d, 0)),
        out_shape=jax.ShapeDtypeStruct((width, total), jnp.bfloat16),
        cost_estimate=pl.CostEstimate(
            flops=2 * tok_count * width * (query_grad.shape[1] + down_grad.shape[1]),
            bytes_accessed=3 * width * total,
            transcendentals=0,
        ),
    )(normed, query_grad, down_grad, up_grad, extra)


def sum_tensor(part):
    if lax.axis_size("tensor") != 2:
        return lax.psum(part, "tensor").astype(jnp.float32)
    part = lax.optimization_barrier(part)
    other = lax.ppermute(part, "tensor", [(0, 1), (1, 0)])
    return part.astype(jnp.float32) + other.astype(jnp.float32)


def local_gathered(
    hidden_in,
    segments,
    expert_ids,
    grad_out,
    attn_gain,
    query_proj,
    latent_down,
    latent_gain,
    latent_up,
    output_proj,
    ffn_gain,
    router_weight,
    shared_gate,
    shared_up,
    shared_down,
    routed_gate_weight,
    routed_up_weight,
    routed_down_weight,
):
    float_type = jnp.float32
    low_type = jnp.bfloat16
    tok_count = hidden_in.shape[0]
    width = hidden_in.shape[1]
    seq_count = segments.shape[0]
    seq_len = segments.shape[1]
    top_count = expert_ids.shape[1]
    head_dim = NOPE + ROPE
    dp_count = lax.axis_size("dp")
    my_dp = lax.axis_index("dp")
    local_experts = routed_gate_weight.shape[0]
    num_experts = router_weight.shape[1]
    capacity = 3 * tok_count * top_count // (2 * num_experts)
    d_part = query_proj.shape[0]
    lat_part = latent_up.shape[0]
    hid_slice = shared_gate.shape[1] // dp_count

    lgain_cols = -(-lat_part // d_part)
    gate_columns = jnp.pad(latent_gain, (0, lgain_cols * d_part - lat_part))
    small_columns = [
        attn_gain.reshape(d_part, 1),
        ffn_gain.reshape(d_part, 1),
        gate_columns.reshape(d_part, lgain_cols),
        router_weight,
        expert_ids.T.reshape(d_part, -1).astype(low_type),
    ]
    big_columns = [query_proj, latent_up.reshape(d_part, -1), latent_down]
    packed = jnp.concatenate(big_columns + small_columns, axis=1)
    packed = jnp.pad(packed, ((0, 0), (0, -packed.shape[1] % 128)))
    packed_all = lax.all_gather(packed, "dp", axis=0, tiled=True)
    shared_send = jnp.concatenate(
        [
            shared_gate.reshape(d_part, dp_count, hid_slice),
            shared_up.reshape(d_part, dp_count, hid_slice),
            shared_down.T.reshape(d_part, dp_count, hid_slice),
        ],
        axis=-1,
    )
    shared_mine = lax.all_to_all(
        jnp.transpose(shared_send, (1, 0, 2)), "dp", split_axis=0, concat_axis=0, tiled=True
    ).reshape(width, 3 * hid_slice)
    cut = width // 512 * 128
    packed_all, shared_mine, output_part = lax.optimization_barrier(
        (packed_all, shared_mine, output_proj.T)
    )
    full_output_t = lax.all_gather(output_part, "dp", axis=0, tiled=True)
    pieces, at = [], 0
    for columns in big_columns + small_columns:
        pieces.append(packed_all[:, at : at + columns.shape[1]])
        at += columns.shape[1]
    full_query, full_up, full_down = pieces[:3]
    full_up = full_up.reshape(-1, latent_up.shape[1])
    full_attn_gain = pieces[3].reshape(-1).astype(float_type)
    full_ffn_gain = pieces[4].reshape(-1).astype(float_type)
    full_lgain = pieces[5].reshape(dp_count, -1)[:, :lat_part].reshape(-1).astype(float_type)
    full_router = pieces[6]
    ids_all = jnp.transpose(
        pieces[7].reshape(dp_count, top_count, tok_count).astype(jnp.int32), (0, 2, 1)
    )
    gate_up_w = shared_mine[:, : 2 * hid_slice]
    down_w_t = shared_mine[:, 2 * hid_slice :]

    def by_seq(array):
        return array.reshape((seq_count, seq_len) + array.shape[1:])

    residual_in = hidden_in.astype(float_type)
    recip_one = rms_recip(residual_in)
    normed_one = (residual_in * recip_one * full_attn_gain).astype(low_type)
    cos_table, sin_table = rope_tables(seq_len, ROPE)
    cos_tok = jnp.tile(cos_table, (seq_count, 1))
    sin_tok = jnp.tile(sin_table, (seq_count, 1))
    head_count = full_query.shape[1] // head_dim
    query_raw = jnp.dot(normed_one, full_query, preferred_element_type=float_type).reshape(
        tok_count, head_count, head_dim
    )
    queries = jnp.concatenate(
        [query_raw[..., :NOPE], rotate(query_raw[..., NOPE:], cos_tok[:, None], sin_tok[:, None])],
        axis=-1,
    ).astype(low_type)
    queries, first_columns = lax.optimization_barrier((queries, grad_out[:, :cut]))
    grad_first = lax.all_gather(first_columns, "dp", axis=0, tiled=True)
    down_raw = jnp.dot(normed_one, full_down, preferred_element_type=float_type)
    latent = down_raw[:, :LAT]
    recip_latent = rms_recip(latent)
    latent_normed = (latent * recip_latent * full_lgain).astype(low_type)
    key_rope = rotate(down_raw[:, LAT:], cos_tok, sin_tok).astype(low_type)
    keys_values = (
        jnp.dot(latent_normed, full_up, preferred_element_type=float_type)
        .astype(low_type)
        .reshape(tok_count, head_count, NOPE + DV)
    )
    key_nope = by_seq(keys_values[..., :NOPE])
    values = by_seq(keys_values[..., NOPE:])
    query_seq = by_seq(queries)
    rope_seq = by_seq(key_rope)
    allowed = mask_table(segments)
    scores = attend_scores(query_seq, key_nope, rope_seq, allowed)
    highest = jnp.max(scores, axis=-1, keepdims=True)
    log_total = highest + jnp.log(jnp.sum(jnp.exp(scores - highest), axis=-1, keepdims=True))
    attn_probs = jnp.exp(scores - log_total)
    probs_low = attn_probs.astype(low_type)
    heads_out = jnp.einsum(
        "shqk,skhd->sqhd", probs_low, values, preferred_element_type=float_type
    ).astype(low_type)
    attn_flat = heads_out.reshape(tok_count, head_count * DV)
    attn_part = lax.dot_general(
        attn_flat, full_output_t, (((1,), (1,)), ((), ())), preferred_element_type=float_type
    )
    attn_full = sum_tensor(attn_part.astype(low_type))
    mid = residual_in + attn_full
    recip_two = rms_recip(mid)
    normed_two = (mid * recip_two * full_ffn_gain).astype(low_type)
    tok_all = lax.all_gather(normed_two, "dp", axis=0, tiled=True)
    tok_all, other_columns = lax.optimization_barrier((tok_all, grad_out[:, cut:]))
    grad_other = lax.all_gather(other_columns, "dp", axis=0, tiled=True)

    logits_all = jnp.dot(tok_all, full_router, preferred_element_type=float_type)
    probs_all = jax.nn.softmax(logits_all, axis=-1)
    router_probs = jax.nn.softmax(
        jnp.dot(normed_two, full_router, preferred_element_type=float_type), axis=-1
    )

    pre_all = jnp.dot(tok_all, gate_up_w, preferred_element_type=float_type)
    shared_pre_up = pre_all[:, hid_slice:]
    shared_act, shared_slope = silu_parts(pre_all[:, :hid_slice])
    shared_hidden = (shared_act * shared_pre_up).astype(low_type)
    split = 2 if lax.axis_size("tensor") == 2 else 1
    turn = lax.axis_index("tensor") if split == 2 else 0

    def own_half_first(array):
        if split == 1:
            return array
        halves = array.reshape((dp_count, 2, tok_count // 2) + array.shape[1:])
        return jnp.where(turn == 0, halves, halves[:, ::-1]).reshape(array.shape)

    ffn_parts, in_grad_part = None, None
    saved = []
    for index in range(local_experts):
        expert = my_dp * local_experts + index
        place = slot_of_token(ids_all, expert, capacity)
        slots = jnp.arange(capacity, dtype=jnp.int32)
        table = place[:, None, :] == slots[None, :, None]
        token_rows = pick_rows(place, [tok_all], capacity)
        column = jnp.sum(
            jnp.where(jnp.arange(num_experts, dtype=jnp.int32) == expert, probs_all, 0.0), axis=-1
        ).reshape(dp_count, 1, tok_count)
        gate_of = jnp.sum(jnp.where(table, column, 0.0), axis=-1).reshape(-1, 1)
        pre_gate = jnp.dot(token_rows, routed_gate_weight[index], preferred_element_type=float_type)
        pre_up = jnp.dot(token_rows, routed_up_weight[index], preferred_element_type=float_type)
        expert_act, expert_slope = silu_parts(pre_gate)
        expert_hidden = (expert_act * pre_up).astype(low_type)
        expert_result = jnp.dot(
            expert_hidden, routed_down_weight[index], preferred_element_type=float_type
        ).astype(low_type)
        left = shared_hidden if index == 0 else jnp.zeros_like(shared_hidden)
        addends = spread_rows(
            own_half_first(place.reshape(-1)).reshape(place.shape),
            expert_result,
            gate_of,
            own_half_first(left),
            down_w_t.T,
            split,
        )
        ffn_parts = addends if index == 0 else [a + b for a, b in zip(ffn_parts, addends)]
        saved.append(
            (place, table, token_rows, gate_of, pre_up, expert_act, expert_slope, expert_hidden)
            + (expert_result,)
        )
    grad_first, grad_other, ffn_parts = lax.optimization_barrier(
        (grad_first, grad_other, ffn_parts)
    )
    if split == 2:
        from_other = lax.ppermute(ffn_parts[1], "tensor", [(0, 1), (1, 0)])
        ffn_half = (ffn_parts[0].astype(float_type) + from_other.astype(float_type)).astype(
            low_type
        )
    else:
        ffn_half = ffn_parts[0]

    shared_act_grad = jnp.dot(
        grad_first, down_w_t[:cut], preferred_element_type=float_type
    ) + jnp.dot(grad_other, down_w_t[cut:], preferred_element_type=float_type)
    shared_grads = jnp.concatenate(
        [shared_act_grad * shared_pre_up * shared_slope, shared_act_grad * shared_act], axis=-1
    ).astype(low_type)

    expert_columns, routed_grads = [], []
    for index in range(local_experts):
        gate_w = routed_gate_weight[index]
        up_w = routed_up_weight[index]
        down_w = routed_down_weight[index]
        place, table, token_rows, gate_of, pre_up, expert_act, expert_slope = saved[index][:7]
        expert_hidden, expert_result = saved[index][7:]
        grad_rows = pick_rows(place, [grad_first, grad_other], capacity).astype(float_type)
        weight_rows = jnp.sum(grad_rows * expert_result.astype(float_type), axis=-1)
        weight_rows = weight_rows.reshape(dp_count, capacity, 1)
        expert_columns.append(jnp.sum(jnp.where(table, weight_rows, 0.0), axis=1))
        slot_grad = (gate_of * grad_rows).astype(low_type)
        hidden_grad = lax.dot_general(
            slot_grad, down_w, (((1,), (1,)), ((), ())), preferred_element_type=float_type
        )
        pre_gate_grad = (hidden_grad * pre_up * expert_slope).astype(low_type)
        pre_up_grad = (hidden_grad * expert_act).astype(low_type)
        row_grad = lax.dot_general(
            pre_gate_grad, gate_w, (((1,), (1,)), ((), ())), preferred_element_type=float_type
        )
        row_grad = row_grad + lax.dot_general(
            pre_up_grad, up_w, (((1,), (1,)), ((), ())), preferred_element_type=float_type
        )
        left = shared_grads if index == 0 else jnp.zeros_like(shared_grads)
        addend = spread_rows(
            place, row_grad.astype(low_type), jnp.ones_like(gate_of), left, gate_up_w.T, 1
        )[0]
        in_grad_part = addend if index == 0 else in_grad_part + addend
        routed_grads.append(
            (
                jnp.dot(token_rows.T, pre_gate_grad, preferred_element_type=float_type),
                jnp.dot(token_rows.T, pre_up_grad, preferred_element_type=float_type),
                jnp.dot(expert_hidden.T, slot_grad, preferred_element_type=float_type),
            )
        )
    routed_out = tuple(jnp.stack(parts) for parts in zip(*routed_grads))

    prob_send = jnp.stack(expert_columns, axis=1)
    prob_part = jnp.transpose(
        lax.all_to_all(prob_send, "dp", split_axis=0, concat_axis=0, tiled=True).reshape(
            num_experts, tok_count
        )
    )
    prob_grad = sum_tensor(prob_part)
    in_grad = lax.psum_scatter(in_grad_part, "dp", scatter_dimension=0, tiled=True)
    shared_gate_up_grad = jnp.dot(tok_all.T, shared_grads, preferred_element_type=float_type)
    shared_down_grad_t = jnp.concatenate(
        [
            jnp.dot(grad_first.T, shared_hidden, preferred_element_type=float_type),
            jnp.dot(grad_other.T, shared_hidden, preferred_element_type=float_type),
        ],
        axis=0,
    )
    shared_back = jnp.concatenate([shared_gate_up_grad, shared_down_grad_t], axis=-1).astype(
        low_type
    )
    in_grad, prob_grad, shared_back, routed_out, ffn_half = lax.optimization_barrier(
        (in_grad, prob_grad, shared_back, routed_out, ffn_half)
    )
    normed_two_grad = sum_tensor(in_grad)
    ffn_sum = lax.psum_scatter(ffn_half, "dp", scatter_dimension=0, tiled=True)
    shared_back = lax.all_to_all(
        shared_back.reshape(dp_count, d_part, 3 * hid_slice),
        "dp",
        split_axis=0,
        concat_axis=0,
        tiled=True,
    )
    shared_back = jnp.transpose(shared_back, (1, 0, 2)).astype(float_type)
    shared_gate_gradient = shared_back[..., :hid_slice].reshape(d_part, -1)
    shared_up_gradient = shared_back[..., hid_slice : 2 * hid_slice].reshape(d_part, -1)
    shared_down_gradient = shared_back[..., 2 * hid_slice :].reshape(d_part, -1).T

    grad_float = grad_out.astype(float_type)
    logit_grad = (
        router_probs * (prob_grad - jnp.sum(prob_grad * router_probs, axis=-1, keepdims=True))
    ).astype(low_type)
    router_weight_gradient = jnp.dot(normed_two.T, logit_grad, preferred_element_type=float_type)
    normed_two_grad = normed_two_grad + jnp.dot(
        logit_grad, full_router.T, preferred_element_type=float_type
    )
    norm_two_back, feedforward_gain_gradient = rms_back(
        normed_two_grad, mid, recip_two, full_ffn_gain
    )
    mid_grad = grad_float + norm_two_back
    mid_low = mid_grad.astype(low_type)
    output_projection_gradient_t = jnp.dot(
        mid_low.T, attn_flat, preferred_element_type=float_type
    )
    heads_grad = by_seq(
        jnp.dot(mid_low, full_output_t, preferred_element_type=float_type)
        .astype(low_type)
        .reshape(tok_count, head_count, DV)
    )
    scale = head_dim ** (-0.5)
    values_grad = jnp.einsum(
        "shqk,sqhd->skhd", probs_low, heads_grad, preferred_element_type=float_type
    )
    probs_grad = jnp.einsum(
        "sqhd,skhd->shqk", heads_grad, values, preferred_element_type=float_type
    )
    delta = jnp.sum(heads_grad.astype(float_type) * heads_out.astype(float_type), axis=-1)
    delta = jnp.transpose(delta, (0, 2, 1))[..., None]
    score_grad = (attn_probs * (probs_grad - delta) * scale).astype(low_type)
    nope_grad_q = jnp.einsum(
        "shqk,skhd->sqhd", score_grad, key_nope, preferred_element_type=float_type
    )
    rope_grad_q = jnp.einsum(
        "shqk,skd->sqhd", score_grad, rope_seq, preferred_element_type=float_type
    )
    key_nope_grad = jnp.einsum(
        "shqk,sqhd->skhd", score_grad, query_seq[..., :NOPE], preferred_element_type=float_type
    )
    key_rope_grad = jnp.einsum(
        "shqk,sqhd->skd", score_grad, query_seq[..., NOPE:], preferred_element_type=float_type
    )
    query_grad = jnp.concatenate([nope_grad_q, rope_grad_q], axis=-1).reshape(
        tok_count, head_count, head_dim
    )
    query_raw_grad = (
        jnp.concatenate(
            [
                query_grad[..., :NOPE],
                rotate(query_grad[..., NOPE:], cos_tok[:, None], -sin_tok[:, None]),
            ],
            axis=-1,
        )
        .astype(low_type)
        .reshape(tok_count, head_count * head_dim)
    )
    kv_grad = (
        jnp.concatenate([key_nope_grad, values_grad], axis=-1)
        .astype(low_type)
        .reshape(tok_count, head_count * (NOPE + DV))
    )
    latent_up_gradient = jnp.dot(latent_normed.T, kv_grad, preferred_element_type=float_type)
    normed_one_part = lax.dot_general(
        query_raw_grad, full_query, (((1,), (1,)), ((), ())), preferred_element_type=float_type
    )
    latent_part_grad = lax.dot_general(
        kv_grad, full_up, (((1,), (1,)), ((), ())), preferred_element_type=float_type
    )
    rope_part_grad = key_rope_grad.reshape(tok_count, ROPE)
    parts = jnp.concatenate(
        [normed_one_part, latent_part_grad, rope_part_grad], axis=-1
    ).astype(low_type)
    sums = sum_tensor(parts)
    normed_one_grad = sums[:, :width]
    latent_normed_grad = sums[:, width : width + LAT]
    rope_key_grad = sums[:, width + LAT :]
    latent_grad, latent_gain_gradient = rms_back(
        latent_normed_grad, latent, recip_latent, full_lgain
    )
    rope_pre_grad = rotate(rope_key_grad, cos_tok, -sin_tok)
    down_grad = jnp.concatenate([latent_grad, rope_pre_grad], axis=-1).astype(low_type)
    normed_one_grad = normed_one_grad + lax.dot_general(
        down_grad, full_down, (((1,), (1,)), ((), ())), preferred_element_type=float_type
    )
    norm_one_back, attention_gain_gradient = rms_back(
        normed_one_grad, residual_in, recip_one, full_attn_gain
    )
    hidden_input_gradient = mid_grad + norm_one_back

    def scatter(array):
        return lax.psum_scatter(
            array.astype(low_type), "dp", scatter_dimension=0, tiled=True
        ).astype(float_type)

    lgain_grad = jnp.pad(
        latent_gain_gradient.reshape(dp_count, lat_part),
        ((0, 0), (0, lgain_cols * d_part - lat_part)),
    )
    columns = [
        attention_gain_gradient.reshape(width, 1),
        feedforward_gain_gradient.reshape(width, 1),
        lgain_grad.reshape(width, lgain_cols),
        router_weight_gradient,
    ]
    small_grads = jnp.concatenate([array.astype(low_type) for array in columns], axis=1)
    down_width = down_grad.shape[1]
    spare = -(down_width + small_grads.shape[1]) % 128
    small_grads = jnp.pad(small_grads, ((0, 0), (down_width, spare)))
    wide_down_grad = jnp.pad(down_grad, ((0, 0), (0, small_grads.shape[1] - down_width)))
    packed_grads = pack_grads(
        normed_one,
        query_raw_grad,
        wide_down_grad,
        latent_up_gradient.astype(low_type),
        small_grads,
        dp_count,
    )
    output_sums = lax.psum_scatter(
        output_projection_gradient_t.astype(low_type), "dp", scatter_dimension=0, tiled=True
    )
    packed_grads, ffn_sum, output_sums = lax.optimization_barrier(
        (packed_grads, ffn_sum, output_sums)
    )
    packed_sums = scatter(packed_grads)
    if split == 2:
        ffn_other = lax.ppermute(ffn_sum, "tensor", [(0, 1), (1, 0)])
        ffn_full = jnp.where(
            turn == 0,
            jnp.concatenate([ffn_sum, ffn_other], axis=0),
            jnp.concatenate([ffn_other, ffn_sum], axis=0),
        ).astype(float_type)
    else:
        ffn_full = sum_tensor(ffn_sum)
    output = (mid + ffn_full).astype(low_type)
    query_width = query_raw_grad.shape[1]
    up_cols = lat_part * latent_up.shape[1] // d_part
    up_sums = packed_sums[:, query_width : query_width + up_cols]
    up_sums = jnp.transpose(up_sums.reshape(-1, lat_part, up_cols), (1, 0, 2))
    at = query_width + up_cols
    down_sums = packed_sums[:, at : at + down_width]
    sums_of, at = [], at + down_width
    for array in columns:
        sums_of.append(packed_sums[:, at : at + array.shape[1]])
        at += array.shape[1]
    return (
        output,
        hidden_input_gradient,
        sums_of[0].reshape(-1),
        packed_sums[:, :query_width],
        down_sums,
        sums_of[2].reshape(-1)[:lat_part],
        up_sums.reshape(lat_part, -1),
        output_sums.astype(float_type).T,
        sums_of[1].reshape(-1),
        sums_of[3],
        shared_gate_gradient,
        shared_up_gradient,
        shared_down_gradient,
    ) + routed_out


def local(*arrays):
    tok_count, top_count = arrays[0].shape[0], arrays[2].shape[1]
    gathered_rows = lax.axis_size("dp") * tok_count
    slot_rows = 3 * tok_count * top_count // 2
    if gathered_rows <= 2 * slot_rows:
        return local_gathered(*arrays)
    return local_exchanged(*arrays)


def solution(mesh):
    return jax.shard_map(
        local,
        mesh=mesh,
        in_specs=(
            P("dp", None),
            P("dp", None),
            P("dp", None),
            P("dp", None),
            P("dp"),
            P("dp", "tensor"),
            P("dp", None),
            P("dp"),
            P("dp", "tensor"),
            P("tensor", "dp"),
            P("dp"),
            P("dp", None),
            P("dp", "tensor"),
            P("dp", "tensor"),
            P("tensor", "dp"),
            P("dp", None, "tensor"),
            P("dp", None, "tensor"),
            P("dp", "tensor", None),
        ),
        out_specs=(
            P("dp", None),
            P("dp", None),
            P("dp"),
            P("dp", "tensor"),
            P("dp", None),
            P("dp"),
            P("dp", "tensor"),
            P("tensor", "dp"),
            P("dp"),
            P("dp", None),
            P("dp", "tensor"),
            P("dp", "tensor"),
            P("tensor", "dp"),
            P("dp", None, "tensor"),
            P("dp", None, "tensor"),
            P("dp", "tensor", None),
        ),
        check_vma=False,
    )
```
